32 devices in a mesh: wave: 8 (over z, y), lev: 4 (over x, core).
Axes of the slice: x: 2, y: 2, z: 4, core: 2. Of those that a mesh axis runs over, the one named last changes fastest.
Arguments:
- spectral: bfloat16 [32, 6, 64, 1280], P('wave', None, 'lev'), may hold values from -0.01171875 to 0.01171875
- legendre: bfloat16 [32, 640, 1280], P('wave'), may hold values from -4 to 4
- wave_ids: int32 [32], replicated, may hold values from 0 to 1279, as said below
- trunc_lengths: int32 [32], replicated, may hold values from 1 to 1280, as said below
- cycle_points: int32 [1280], replicated, may hold values from 20 to 2560, as said below
- grid_coef: float32 [1280, 2560], P('wave'), may hold values from -6 to 6
- cycle_weights: float32 [640], replicated, may hold values from 0.1 to 2
- modes_in: bfloat16 [64, 64], replicated, may hold values from -0.75 to 0.75
- modes_out: bfloat16 [64, 64], replicated, may hold values from -0.75 to 0.75
- depths: float32 [64], replicated, may hold values from 0.05 to 20
Outputs:
- update: bfloat16 [32, 6, 64, 1280], P('wave', None, 'lev')
The draws below stay inside these ranges and needn't reach their ends.
Inputs may be any that keep to these rules, and one draw needn't show every extreme that they name: `wave_ids`: distinct zonal wavenumbers; one slot holds wavenumber 0. `trunc_lengths`: the length of slot m is at most 1280 minus wave_ids[m] and at least half of that; the slot of wavenumber 0 has length 1280. `cycle_points`: multiples of 4; cycle j and cycle 1280 - 1-j have the same count; cycles near the equator have 2560.
All inputs are finite; a program needn't handle non-finite values.
Results may differ from the reference program's by a relative error of at most 0.011.
Values may be sent and summed in bfloat16 or wider, within the bound.
A program may use at most 128 MiB of HBM per device.

```python
import math
import jax
import jax.numpy as jnp
from jax import lax

NT = 1280
NLAT = 1280
NHALF = 640
LONMAX = 2560
FIELDS = 3
M_WIN = 32
LEVELS = 64


def wave_table(key):
    base_key = jax.random.fold_in(key, 11)
    others = jax.random.permutation(jax.random.fold_in(base_key, 1), NT - 1)[:M_WIN - 1] + 1
    chosen = jnp.concatenate([jnp.zeros((1,), jnp.int32), others.astype(jnp.int32)])
    shuffle = jax.random.permutation(jax.random.fold_in(base_key, 2), M_WIN)
    waves = chosen[shuffle]
    jitter = jax.random.randint(jax.random.fold_in(base_key, 3), (M_WIN,), 0, 4)
    jitter = jnp.where(waves == 0, 0, jitter)
    headroom = NT - waves
    shorten = jnp.minimum(8 * jitter, headroom // 2)
    return (waves.astype(jnp.int32), (headroom - shorten).astype(jnp.int32))


def draw_wave_ids(key, part):
    return wave_table(key)[0]


def draw_trunc_lengths(key, part):
    return wave_table(key)[1]


def draw_cycle_points(key, part):
    cycle_index = jnp.arange(NHALF, dtype=jnp.int32)
    jitter = jax.random.randint(jax.random.fold_in(key, 21), (NHALF,), 0, 4)
    northern = jnp.minimum(LONMAX, 20 + 4 * cycle_index + 4 * jitter)
    return jnp.concatenate([northern, northern[::-1]]).astype(jnp.int32)


def levels(key, extent, shards, least, high):
    def one(dim, blocks):
        heights = jax.random.uniform(jax.random.fold_in(jax.random.fold_in(key, 6), dim), (blocks,), jnp.float32, least / len(shards), high / len(shards))
        return jnp.repeat(jnp.exp(heights), extent[dim] // blocks).reshape((-1,) + (1,) * (len(extent) - dim - 1))

    gain = one(*shards[0])
    for cut in shards[1:]:
        gain = gain * one(*cut)
    return gain


def noise(stream_key, dims, width, bound, split=(), kind=jnp.bfloat16):
    values = width * jax.random.normal(stream_key, dims, jnp.float32)
    if split:
        values = values * levels(stream_key, dims, split, -0.22, 0.18)
    return jnp.clip(values, -bound, bound).astype(kind)


def setup_inputs(seed: int = 0) -> dict:
    keys = jax.random.split(jax.random.key(seed), 11)
    spectral = noise(keys[0], (M_WIN, 2 * FIELDS, LEVELS, NT), 0.002, 0.01171875, ((0, 8), (2, 4)))
    legendre = noise(keys[1], (M_WIN, NHALF, NT), 1.0, 4.0, ((0, 8),))
    wave_ids = draw_wave_ids(jax.random.fold_in(keys[10], 71), 0)
    trunc_lengths = draw_trunc_lengths(jax.random.fold_in(keys[10], 71), 0)
    cycle_points = draw_cycle_points(jax.random.fold_in(keys[10], 71), 0)
    grid_coef = noise(keys[5], (NLAT, LONMAX), 1.0, 6.0, ((0, 8),), jnp.float32)
    cycle_weights = jnp.clip(jnp.exp(jax.random.uniform(keys[6], (NHALF,), jnp.float32, math.log(0.1), math.log(2.0))), 0.1, 2.0)
    modes_in = noise(keys[7], (LEVELS, LEVELS), LEVELS ** -0.5, 0.75)
    modes_out = noise(keys[8], (LEVELS, LEVELS), LEVELS ** -0.5, 0.75)
    depths = jnp.clip(jnp.exp(jax.random.uniform(keys[9], (LEVELS,), jnp.float32, math.log(0.05), math.log(20.0))), 0.05, 20.0)
    return {"spectral": spectral, "legendre": legendre, "wave_ids": wave_ids, "trunc_lengths": trunc_lengths, "cycle_points": cycle_points, "grid_coef": grid_coef, "cycle_weights": cycle_weights, "modes_in": modes_in, "modes_out": modes_out, "depths": depths}


def trig_rows(wave_ids, cycle_count, lon_max):
    longitude = jnp.arange(lon_max, dtype=jnp.int32)
    counts = cycle_count[:, None, None]
    phase_idx = (wave_ids[None, :, None] * longitude[None, None, :]) % counts
    angles = (2.0 * jnp.pi) * phase_idx.astype(jnp.float32) / counts.astype(jnp.float32)
    live_mask = (longitude[None, None, :] < counts) & (2 * wave_ids[None, :, None] < counts)
    cosine = jnp.where(live_mask, jnp.cos(angles), 0.0)
    sine_part = jnp.where(live_mask, -jnp.sin(angles), 0.0)
    return jnp.stack([cosine, sine_part], axis=1).astype(jnp.bfloat16)


def cycle_trip(fourier, wave_ids, cycle_count, coef_rows):
    wave_total, channels, items, group_size = fourier.shape
    fields = channels // 2
    polys = trig_rows(wave_ids, cycle_count, coef_rows.shape[1])
    factor = jnp.where(wave_ids == 0, 1.0, 2.0).astype(jnp.bfloat16)
    weighted = (fourier * factor[:, None, None, None]).reshape(wave_total, 2, fields, items, group_size)
    grid_vals = jnp.einsum("mrfig,grmk->gfik", weighted.astype(jnp.float32), polys.astype(jnp.float32))
    tendency = (grid_vals * (coef_rows[:, None, None, :] + jnp.roll(grid_vals, -1, axis=1))).astype(jnp.bfloat16)
    analysed = jnp.einsum("gfik,grmk->mrfig", tendency.astype(jnp.float32), polys.astype(jnp.float32))
    analysed = analysed / cycle_count.astype(jnp.float32)
    return analysed.astype(jnp.bfloat16).reshape(wave_total, channels, items, group_size)


def reference(spectral, legendre, wave_ids, trunc_lengths, cycle_points, grid_coef, cycle_weights, modes_in, modes_out, depths):
    wave_total, channels, levels_total, spec_len = spectral.shape
    half_lat = legendre.shape[1]
    lat_total = 2 * half_lat
    position = jnp.arange(spec_len, dtype=jnp.int32)
    parity_sign = jnp.where(position % 2 == 0, 1.0, -1.0).astype(jnp.bfloat16)

    def inverse_one(packed):
        coeffs, polys, length = packed
        flat = coeffs.reshape(-1, spec_len)
        flat = jnp.where(position[None, :] < length, flat, jnp.zeros_like(flat))
        northern = jnp.dot(flat, polys.T, preferred_element_type=jnp.float32)
        southern = jnp.dot(flat * parity_sign[None, :], polys.T, preferred_element_type=jnp.float32)
        joined = jnp.concatenate([northern, jnp.flip(southern, axis=1)], axis=1).astype(jnp.bfloat16)
        return joined.reshape(channels, levels_total, lat_total)

    fourier = lax.map(inverse_one, (spectral, legendre, trunc_lengths))

    group_size = math.gcd(lat_total, 32)
    groups = lat_total // group_size
    stacked = jnp.moveaxis(fourier.reshape(wave_total, channels, levels_total, groups, group_size), 3, 0)
    counts = cycle_points.reshape(groups, group_size)
    coefs = grid_coef.reshape(groups, group_size, -1)

    def group_trip(packed):
        return cycle_trip(packed[0], wave_ids, packed[1], packed[2])

    results = lax.map(group_trip, (stacked, counts, coefs))
    returned = jnp.moveaxis(results, 0, 3).reshape(wave_total, channels, levels_total, lat_total)

    def forward_one(packed):
        values, polys, length, wavenum = packed
        northern = values[..., :half_lat].astype(jnp.float32)
        southern = jnp.flip(values[..., half_lat:], axis=2).astype(jnp.float32)
        even_part = (cycle_weights * (northern + southern)).astype(jnp.bfloat16).reshape(-1, half_lat)
        odd_part = (cycle_weights * (northern - southern)).astype(jnp.bfloat16).reshape(-1, half_lat)
        from_even = jnp.dot(even_part, polys, preferred_element_type=jnp.float32)
        from_odd = jnp.dot(odd_part, polys, preferred_element_type=jnp.float32)
        coeffs = jnp.where(position[None, :] % 2 == 0, from_even, from_odd)
        coeffs = jnp.where(position[None, :] < length, coeffs, 0.0).astype(jnp.bfloat16)
        coeffs = coeffs.reshape(channels, levels_total, spec_len)
        mode_vals = jnp.einsum("kl,cli->cki", modes_in.astype(jnp.float32), coeffs.astype(jnp.float32))
        degree = (wavenum + position).astype(jnp.float32)
        damp = 1.0 / (1.0 + depths[:, None] * degree[None, :] * (degree[None, :] + 1.0) / float(NT * NT))
        scaled = (mode_vals * damp[None, :, :]).astype(jnp.bfloat16)
        mixed = jnp.einsum("lk,cki->cli", modes_out.astype(jnp.float32), scaled.astype(jnp.float32))
        return mixed.astype(jnp.bfloat16)

    return lax.map(forward_one, (returned, legendre, trunc_lengths, wave_ids))
```

```python
import functools

import jax
import jax.numpy as jnp
import numpy as np
from jax import lax
from jax.experimental import pallas as pl
from jax.experimental.pallas import tpu as pltpu
from jax.sharding import PartitionSpec as P

NT = 1280
LOW = 256
LANES = 128
GROUP = 8
NN = (((1,), (0,)), ((), ()))
NTD = (((1,), (1,)), ((), ()))
TN = (((0,), (0,)), ((), ()))
F32 = jnp.float32
BF16 = jnp.bfloat16


def turn_coefs(func, degree):
    nodes = 0.125 * (1.0 + np.cos(np.pi * (np.arange(degree + 1) + 0.5) / (degree + 1)))
    cheb = np.polynomial.Chebyshev.fit(nodes, func(nodes), degree, domain=[0.0, 0.25])
    return [float(v) for v in cheb.convert(kind=np.polynomial.Polynomial).coef]


COS = turn_coefs(lambda u: np.cos(2 * np.pi * np.sqrt(u)), 5)
SIN = turn_coefs(lambda u: np.sin(2 * np.pi * np.sqrt(u)) / np.sqrt(u), 5)


def horner(coefs, u):
    total = jnp.full_like(u, coefs[-1])
    for value in coefs[-2::-1]:
        total = total * u + value
    return total


def turns(product, points, inverse):
    return (product - jnp.round(product * inverse) * points) * inverse


def pad_to(value, unit):
    return -(-value // unit) * unit


def join_lanes(pieces, width):
    lane = lax.broadcasted_iota(jnp.int32, pieces[0].shape, 1)
    total = pad_to(len(pieces) * width, LANES) // LANES
    outs = [None] * total
    for no, piece in enumerate(pieces):
        seat, low = divmod(no * width, LANES)
        moved = pltpu.roll(piece, low, 1) if low else piece
        outs[seat] = moved if low == 0 else jnp.where(lane >= low, moved, outs[seat])
        if low + width > LANES:
            outs[seat + 1] = moved
    return jnp.concatenate(outs, axis=1)


def take_lanes(block, no, width):
    seat, low = divmod(no * width, LANES)
    piece = block[:, seat * LANES : (seat + 1) * LANES]
    if low + width > LANES:
        lane = lax.broadcasted_iota(jnp.int32, piece.shape, 1)
        piece = jnp.where(lane >= low, piece, block[:, (seat + 1) * LANES : (seat + 2) * LANES])
    return pltpu.roll(piece, LANES - low, 1) if low else piece


def inverse_kernel(lengths, spec_ref, leg_ref, out_ref, both_ref):
    shards, band, _ = out_ref.shape
    waves, channels, items, span = spec_ref.shape
    rows = channels * items
    wide = both_ref.shape[1] // 2
    part = pl.program_id(0)

    @pl.when(part == 0)
    def _():
        for m in range(waves):
            coeffs = spec_ref[m].reshape(rows, span)
            place = lax.broadcasted_iota(jnp.int32, (rows, span), 1)
            live = jnp.where(place < lengths[m], coeffs.astype(F32), 0.0)
            sign = jnp.where(place % 2 == 0, live, -live).astype(BF16)
            live = live.astype(BF16)
            fill = jnp.zeros((wide - rows, span), BF16)
            both_ref[m] = jnp.concatenate([live, fill, sign, fill], axis=0)

    north, south = [], []
    for m in range(waves):
        sums = lax.dot_general(leg_ref[m], both_ref[m], NTD, preferred_element_type=F32)
        north.append(sums[:, :wide])
        south.append(sums[:, wide:])
    out_ref[part] = join_lanes(north, rows).astype(BF16)
    out_ref[shards - 1 - part] = join_lanes(south, rows).astype(BF16)


def inverse_legendre(spectral, legendre, lengths, shards):
    waves, channels, items, span = spectral.shape
    half_lat = legendre.shape[1]
    band = 2 * half_lat // shards
    rows = channels * items
    lanes = pad_to(waves * rows, LANES)
    wide = pad_to(rows, LANES)
    return pl.pallas_call(
        inverse_kernel,
        name="inverse",
        out_shape=jax.ShapeDtypeStruct((shards, band, lanes), BF16),
        grid_spec=pltpu.PrefetchScalarGridSpec(
            num_scalar_prefetch=1,
            grid=(shards // 2,),
            in_specs=[
                pl.BlockSpec((waves, channels, items, span), lambda k, s: (0, 0, 0, 0)),
                pl.BlockSpec((waves, band, span), lambda k, s: (0, k, 0)),
            ],
            out_specs=pl.BlockSpec((shards, band, lanes), lambda k, s: (0, 0, 0)),
            scratch_shapes=[pltpu.VMEM((waves, 2 * wide, span), BF16)],
        ),
        compiler_params=pltpu.CompilerParams(vmem_limit_bytes=40 << 20),
        cost_estimate=pl.CostEstimate(
            flops=4 * waves * rows * half_lat * span,
            bytes_accessed=2 * waves * half_lat * span,
            transcendentals=0,
        ),
    )(lengths, spectral, legendre)


def forward_kernel(lengths, values_ref, leg_ref, weight_ref, out_ref):
    shards, band, lanes = values_ref.shape
    rows = out_ref.shape[1]
    half = shards // 2
    span = leg_ref.shape[2]
    turn = pl.program_id(0)
    length = lengths[turn]
    seat = turn * rows // LANES
    low = turn * rows % LANES
    after = jnp.minimum(seat + 1, lanes // LANES - 1)

    def side(order):
        here, there = [
            jnp.concatenate([values_ref[k, :, pl.ds(v * LANES, LANES)] for k in order], axis=0)
            for v in (seat, after)
        ]
        lane = lax.broadcasted_iota(jnp.int32, here.shape, 1)
        piece = jnp.where(lane >= low, here.astype(F32), there.astype(F32))
        return pltpu.roll(piece, LANES - low, 1)[:, :rows]

    north = side(range(half))
    south = side([shards - 1 - k for k in range(half)])
    weights = weight_ref[:, :1]
    even = (weights * (north + south)).astype(BF16)
    odd = (weights * (north - south)).astype(BF16)
    polys = leg_ref[0]
    from_even = lax.dot_general(even, polys, TN, preferred_element_type=F32)
    from_odd = lax.dot_general(odd, polys, TN, preferred_element_type=F32)
    place = lax.broadcasted_iota(jnp.int32, (rows, span), 1)
    values = jnp.where(place % 2 == 0, from_even, from_odd)
    out_ref[0] = jnp.where(place < length, values, 0.0).astype(BF16)


def forward_legendre(returned, legendre, lengths, weights, rows):
    shards, band, lanes = returned.shape
    waves, half_lat, span = legendre.shape
    spread = jnp.broadcast_to(weights[:, None], (half_lat, LANES))
    return pl.pallas_call(
        forward_kernel,
        name="forward",
        out_shape=jax.ShapeDtypeStruct((waves, rows, span), BF16),
        grid_spec=pltpu.PrefetchScalarGridSpec(
            num_scalar_prefetch=1,
            grid=(waves,),
            in_specs=[
                pl.BlockSpec((shards, band, lanes), lambda m, s: (0, 0, 0)),
                pl.BlockSpec((1, half_lat, span), lambda m, s: (m, 0, 0)),
                pl.BlockSpec((half_lat, LANES), lambda m, s: (0, 0)),
            ],
            out_specs=pl.BlockSpec((1, rows, span), lambda m, s: (m, 0, 0)),
        ),
        compiler_params=pltpu.CompilerParams(vmem_limit_bytes=40 << 20),
        cost_estimate=pl.CostEstimate(
            flops=4 * waves * rows * half_lat * span,
            bytes_accessed=2 * waves * half_lat * span,
            transcendentals=0,
        ),
    )(lengths, returned, legendre, spread)


def exchange_kernel(
    fields,
    chunk,
    points,
    inverses,
    sent_ref,
    coef_ref,
    lane_ref,
    wave_ref,
    pick_ref,
    merge_ref,
    back_ref,
    land_ref,
    leave_ref,
    in_ref,
    out_ref,
    in_send,
    in_recv,
    out_send,
    out_recv,
    own_sems,
):
    shards, band, _ = sent_ref.shape
    waves = wave_ref.shape[0]
    local_waves = waves // shards
    both_rows = 2 * pick_ref.shape[0]
    rows = both_rows // 2
    items = rows // fields
    lon_max = coef_ref.shape[1]
    chunks = lon_max // LOW
    steps = pad_to(chunks, 8)
    wide = 4 * waves
    me = lax.axis_index("wave")
    reverse = (me * 2) // shards

    barrier = pltpu.get_barrier_semaphore()
    for away in range(1, shards):
        pl.semaphore_signal(
            barrier,
            inc=1,
            device_id={"wave": lax.rem(me + away, shards)},
            device_id_type=pl.DeviceIdType.MESH,
        )
    pl.semaphore_wait(barrier, shards - 1)

    def span_of(part):
        return pl.ds(pl.multiple_of(part * chunk, chunk), chunk)

    def remote(src, dst, send, recv, away, part):
        to = lax.rem(me + away, shards)
        return pltpu.make_async_remote_copy(
            src_ref=src.at[to, span_of(part), :],
            dst_ref=dst.at[me, span_of(part), :],
            send_sem=send.at[away - 1, part],
            recv_sem=recv.at[away - 1, part],
            device_id={"wave": to},
            device_id_type=pl.DeviceIdType.MESH,
        )

    def own(src, dst, which, part):
        return pltpu.make_async_copy(
            src.at[me, span_of(part), :],
            dst.at[me, span_of(part), :],
            own_sems.at[which, part],
        )

    def start_in(part, carry):
        for away in range(1, shards):
            remote(sent_ref, land_ref, in_send, in_recv, away, part).start()
        own(sent_ref, land_ref, 0, part).start()
        return carry

    lax.fori_loop(0, band // chunk, start_in, 0)

    wave_lane = lane_ref[0:1, :]
    step_no = lax.broadcasted_iota(jnp.int32, (steps, wide), 0).astype(F32)
    step_wave = step_no * (wave_lane * float(LOW))
    low_no = lax.broadcasted_iota(jnp.int32, (waves, LANES), 1)
    low_wave = low_no.astype(F32) * wave_ref[...]
    row_lane = lax.broadcasted_iota(jnp.int32, (waves, LANES), 1)
    out_lane = lax.broadcasted_iota(jnp.int32, (rows, 2 * waves), 1)
    place = lax.broadcasted_iota(jnp.int32, (1, LOW), 1).astype(F32)

    def prepare(local):
        pts = points[local]
        inv = inverses[local]
        step = turns(step_wave, pts, inv) - lane_ref[1:2, :]
        step = step - jnp.round(step)
        signs = jnp.where(2.0 * wave_lane < pts, lane_ref[2:3, :], 0.0)
        anal = horner(COS, step * step) * signs
        synth = anal * lane_ref[3:4, :]
        turn = turns(low_wave, pts, inv)
        square = turn * turn
        cos_low = horner(COS, square)
        sin_low = horner(SIN, square) * turn
        half = LANES // 2
        cos_half = jnp.broadcast_to(cos_low[:, half : half + 1], cos_low.shape)
        sin_half = jnp.broadcast_to(sin_low[:, half : half + 1], sin_low.shape)
        twice = cos_half + cos_half
        cos_full = twice * cos_half - 1.0
        sin_full = twice * sin_half
        cos_far = cos_low * cos_full - sin_low * sin_full
        sin_far = sin_low * cos_full + cos_low * sin_full
        cos_all = jnp.concatenate([cos_low.astype(BF16), cos_far.astype(BF16)], axis=1)
        sin_all = jnp.concatenate([sin_low.astype(BF16), sin_far.astype(BF16)], axis=1)
        return pts, inv, synth, anal, cos_all, sin_all

    def pick(seat):
        data = jnp.concatenate(
            [in_ref[w, pl.ds(seat, shards, stride=chunk), :] for w in range(local_waves)], axis=0
        )
        real = jnp.where(row_lane < rows, data, 0.0).astype(BF16)
        other = (row_lane >= rows) & (row_lane < both_rows)
        imag = jnp.where(other, data, 0.0).astype(BF16)
        four = jnp.concatenate([real, imag, imag, real], axis=0)
        spread = lax.dot_general(pick_ref[...], four, NTD, preferred_element_type=F32)
        return spread.astype(BF16)

    def tendency(grid, local, pts):
        pieces = []
        for k in range(chunks):
            vals = grid[k * rows : (k + 1) * rows].astype(BF16)
            after = jnp.concatenate([vals[items:], vals[:items]], axis=0)
            coef = coef_ref[pl.ds(local, 1), k * LOW : (k + 1) * LOW]
            coef = jnp.broadcast_to(coef, (items, LOW)).astype(BF16)
            coef = jnp.concatenate([coef] * fields, axis=0)
            tend = vals * (coef + after)
            live = jnp.broadcast_to(place < pts - float(k * LOW), tend.shape)
            pieces.append(jnp.where(live, tend, jnp.zeros_like(tend)))
        return jnp.concatenate(pieces, axis=0)

    def reduce(back, anal, inv):
        total = back[:rows] * anal[0:1, :]
        for k in range(1, chunks):
            total = total + back[k * rows : (k + 1) * rows] * anal[k : k + 1, :]
        result = (total[:, : 2 * waves] + total[:, 2 * waves :]) * inv
        return jnp.concatenate(
            [
                jnp.where(out_lane < waves, result, 0.0).astype(BF16),
                jnp.where(out_lane < waves, 0.0, result).astype(BF16),
                jnp.zeros((LANES - both_rows, 2 * waves), BF16),
            ],
            axis=0,
        )

    def stretch(row):
        block = jnp.broadcast_to(row, (items, wide)).astype(BF16)
        return jnp.concatenate([block] * fields, axis=0)

    def several(part, step, carry):
        seats = [step * GROUP + g for g in range(GROUP)]
        stored = [part * chunk + v for v in seats]
        locals_ = [v + reverse * (band - 1 - 2 * v) for v in stored]
        made = [prepare(v) for v in locals_]
        spreads = [pick(v) for v in seats]
        turned = [
            jnp.concatenate(
                [x * stretch(w[2][k : k + 1, :]) for k in range(chunks)], axis=0
            )
            for x, w in zip(spreads, made)
        ]
        grids = [
            lax.dot_general(
                x,
                jnp.concatenate([w[4], w[5], w[4], w[5]], axis=0),
                NN,
                preferred_element_type=F32,
            )
            for x, w in zip(turned, made)
        ]
        tends = [tendency(x, v, w[0]) for x, v, w in zip(grids, locals_, made)]
        backs = [
            lax.dot_general(
                x,
                jnp.concatenate([w[4], w[5], w[5], w[4]], axis=0),
                NTD,
                preferred_element_type=F32,
            )
            for x, w in zip(tends, made)
        ]
        splits = [reduce(x, w[3], w[1]) for x, w in zip(backs, made)]
        outs = [
            lax.dot_general(merge_ref[...], x, NTD, preferred_element_type=F32)
            for x in splits
        ]
        for seat, value in zip(seats, outs):
            for w in range(local_waves):
                out_ref[w, pl.ds(seat, shards, stride=chunk), :] = value[w * shards : (w + 1) * shards]
        return carry

    def work(part, carry):
        for away in range(1, shards):
            remote(sent_ref, land_ref, in_send, in_recv, away, part).wait_recv()
        own(sent_ref, land_ref, 0, part).wait()
        got = land_ref[:, span_of(part), :].astype(F32).reshape(shards * chunk, -1)
        for w in range(local_waves):
            in_ref[w] = take_lanes(got, w, both_rows)
        lax.fori_loop(0, chunk // GROUP, functools.partial(several, part), 0)
        made = join_lanes([out_ref[w] for w in range(local_waves)], both_rows).astype(BF16)
        leave_ref[:, span_of(part), :] = made.reshape(shards, chunk, -1)
        for away in range(1, shards):
            remote(leave_ref, back_ref, out_send, out_recv, away, part).start()
        own(leave_ref, back_ref, 1, part).start()
        return carry

    lax.fori_loop(0, band // chunk, work, 0)

    def finish(part, carry):
        for away in range(1, shards):
            remote(sent_ref, land_ref, in_send, in_recv, away, part).wait_send()
            remote(leave_ref, back_ref, out_send, out_recv, away, part).wait()
        own(leave_ref, back_ref, 1, part).wait()
        return carry

    lax.fori_loop(0, band // chunk, finish, 0)


def cycle_trips(values, wave_ids, points, coef, fields, both_rows):
    shards, band, _ = values.shape
    waves = wave_ids.shape[0]
    local_waves = waves // shards
    rows = both_rows // 2
    wide = 4 * waves
    lon_max = coef.shape[1]
    chunk = next(c for c in (16, 8) if band % c == 0)
    parts = band // chunk
    wave_ids = wave_ids.reshape(shards, local_waves).T.reshape(-1)
    lane = jnp.arange(wide)
    part = lane // waves
    wave_lane = jnp.tile(wave_ids, 4).astype(F32)
    factor = jnp.where(wave_lane == 0, 1.0, 2.0)
    quarter = jnp.where(part < 2, 0.0, 0.25)
    signs = jnp.where(part == 0, 1.0, -1.0)
    zero = jnp.zeros_like(factor)
    lanes = jnp.stack([wave_lane, quarter, signs, factor, zero, zero, zero, zero], axis=0)
    wave_col = jnp.broadcast_to(wave_ids.astype(F32)[:, None], (waves, LANES))
    lanes_in = jnp.arange(LANES)[None, :]
    pick = (jnp.arange(rows)[:, None] == lanes_in % rows) & (lanes_in < both_rows)
    pick = pick.astype(BF16)
    merge = (jnp.arange(waves)[:, None] == jnp.arange(2 * waves)[None, :] % waves).astype(BF16)

    vmem = pl.BlockSpec(memory_space=pltpu.VMEM)
    smem = pl.BlockSpec(memory_space=pltpu.SMEM)
    dma = pltpu.SemaphoreType.DMA
    return pl.pallas_call(
        functools.partial(exchange_kernel, fields, chunk),
        name="cycles",
        out_shape=jax.ShapeDtypeStruct(values.shape, BF16),
        in_specs=[smem, smem] + [vmem] * 6,
        out_specs=vmem,
        scratch_shapes=[
            pltpu.VMEM(values.shape, BF16),
            pltpu.VMEM(values.shape, BF16),
            pltpu.VMEM((local_waves, shards * chunk, LANES), F32),
            pltpu.VMEM((local_waves, shards * chunk, LANES), F32),
            dma((shards - 1, parts)),
            dma((shards - 1, parts)),
            dma((shards - 1, parts)),
            dma((shards - 1, parts)),
            dma((2, parts)),
        ],
        compiler_params=pltpu.CompilerParams(
            vmem_limit_bytes=30 << 20, collective_id=0, has_side_effects=True
        ),
        cost_estimate=pl.CostEstimate(
            flops=8 * band * waves * rows * lon_max,
            bytes_accessed=4 * band * lon_max,
            transcendentals=0,
        ),
    )(
        points.astype(F32),
        1.0 / points.astype(F32),
        values,
        coef,
        lanes,
        wave_col,
        pick,
        merge,
    )


def level_kernel(
    channels,
    levs,
    ids,
    own_ref,
    in_ref,
    out_modes_ref,
    depth_ref,
    update_ref,
    all_ref,
    far_send,
    far_recv,
    near_send,
    near_recv,
    own_sems,
):
    waves, rows, span = own_ref.shape
    items = rows // channels
    modes = in_ref.shape[0]
    chips = levs // 2
    me = lax.axis_index("lev")
    chip, core = me // 2, lax.rem(me, 2)
    partner = chip * 2 + 1 - core

    barrier = pltpu.get_barrier_semaphore()
    peers = [lax.rem(chip + d, chips) * 2 + core for d in range(1, chips)]
    for peer in peers + [partner]:
        pl.semaphore_signal(
            barrier, inc=1, device_id={"lev": peer}, device_id_type=pl.DeviceIdType.MESH
        )
    pl.semaphore_wait(barrier, chips)

    def far(away, m):
        return pltpu.make_async_remote_copy(
            src_ref=own_ref.at[m],
            dst_ref=all_ref.at[me, m],
            send_sem=far_send.at[away - 1, m],
            recv_sem=far_recv.at[away - 1, m],
            device_id={"lev": peers[away - 1]},
            device_id_type=pl.DeviceIdType.MESH,
        )

    def near(away, m):
        owner = lax.rem(chip + chips - away, chips) * 2 + core
        return pltpu.make_async_remote_copy(
            src_ref=own_ref.at[m] if away == 0 else all_ref.at[owner, m],
            dst_ref=all_ref.at[owner, m],
            send_sem=near_send.at[away, m],
            recv_sem=near_recv.at[away, m],
            device_id={"lev": partner},
            device_id_type=pl.DeviceIdType.MESH,
        )

    def own(m):
        return pltpu.make_async_copy(own_ref.at[m], all_ref.at[me, m], own_sems.at[m])

    for m in range(waves):
        for away in range(1, chips):
            far(away, m).start()
        near(0, m).start()
        own(m).start()

    def solve(m):
        own(m).wait()
        for away in range(chips):
            near(away, m).wait_recv()
        place = lax.broadcasted_iota(jnp.int32, (modes, span), 1)
        degree = (place + ids[m]).astype(F32)
        damp = 1.0 / (1.0 + depth_ref[:, :1] * degree * (degree + 1.0) / float(NT * NT))
        for c in range(channels):
            stack = jnp.concatenate(
                [all_ref[s, m, c * items : (c + 1) * items, :] for s in range(levs)], axis=0
            )
            vals = lax.dot_general(in_ref[...], stack, NN, preferred_element_type=F32)
            scaled = (vals * damp).astype(BF16)
            update_ref[m, c] = lax.dot_general(
                out_modes_ref[...], scaled, NN, preferred_element_type=F32
            ).astype(BF16)

    for m in range(waves):
        for away in range(1, chips):
            far(away, m).wait_recv()
            near(away, m).start()
        if m > 0:
            solve(m - 1)
    solve(waves - 1)
    for m in range(waves):
        for away in range(1, chips):
            far(away, m).wait_send()
        for away in range(chips):
            near(away, m).wait_send()


def vertical(projected, modes_in, own_rows, depths, own_waves, channels, levs):
    waves, rows, span = projected.shape
    items = rows // channels
    modes = modes_in.shape[0]
    chips = levs // 2
    spread = jnp.broadcast_to(depths[:, None], (modes, LANES))
    vmem = pl.BlockSpec(memory_space=pltpu.VMEM)
    dma = pltpu.SemaphoreType.DMA
    return pl.pallas_call(
        functools.partial(level_kernel, channels, levs),
        name="vertical",
        out_shape=jax.ShapeDtypeStruct((waves, channels, items, span), BF16),
        in_specs=[pl.BlockSpec(memory_space=pltpu.SMEM)] + [vmem] * 4,
        out_specs=vmem,
        scratch_shapes=[
            pltpu.VMEM((levs, waves, rows, span), BF16),
            dma((max(chips - 1, 1), waves)),
            dma((max(chips - 1, 1), waves)),
            dma((chips, waves)),
            dma((chips, waves)),
            dma((waves,)),
        ],
        compiler_params=pltpu.CompilerParams(
            vmem_limit_bytes=40 << 20, collective_id=1, has_side_effects=True
        ),
    )(own_waves, projected, modes_in, own_rows, spread)


def on_device(
    spectral,
    legendre,
    wave_ids,
    trunc_lengths,
    cycle_points,
    grid_coef,
    cycle_weights,
    modes_in,
    modes_out,
    depths,
):
    wave_rank = lax.axis_index("wave")
    lev_rank = lax.axis_index("lev")
    shards = lax.axis_size("wave")
    waves, channels, items, span = spectral.shape
    rows = channels * items
    band = grid_coef.shape[0]
    own_waves = lax.dynamic_slice_in_dim(wave_ids, wave_rank * waves, waves)
    own_lengths = lax.dynamic_slice_in_dim(trunc_lengths, wave_rank * waves, waves)
    fourier = inverse_legendre(spectral, legendre, own_lengths, shards)
    points = lax.dynamic_slice_in_dim(cycle_points, wave_rank * band, band)
    returned = cycle_trips(fourier, wave_ids, points, grid_coef, channels // 2, rows)
    projected = forward_legendre(returned, legendre, own_lengths, cycle_weights, rows)
    own_rows = lax.dynamic_slice_in_dim(modes_out, lev_rank * items, items, 0)
    levs = lax.axis_size("lev")
    return vertical(projected, modes_in, own_rows, depths, own_waves, channels, levs)


def solution(mesh):
    placed = (
        P("wave", None, "lev", None),
        P("wave", None, None),
        P(),
        P(),
        P(),
        P("wave", None),
        P(),
        P(),
        P(),
        P(),
    )
    return jax.shard_map(
        on_device,
        mesh=mesh,
        in_specs=placed,
        out_specs=P("wave", None, "lev", None),
        check_vma=False,
    )
```

```python
import functools

import jax
import jax.numpy as jnp
import numpy as np
from jax import lax
from jax.experimental import pallas as pl
from jax.experimental.pallas import tpu as pltpu
from jax.sharding import PartitionSpec as P

NT = 1280
LOW = 256
LANES = 128
GROUP = 8
LEAD = 2
FIRST = 3
SECOND = 5
NN = (((1,), (0,)), ((), ()))
NTD = (((1,), (1,)), ((), ()))
F32 = jnp.float32
BF16 = jnp.bfloat16


def turn_coefs(func, degree):
    nodes = 0.125 * (1.0 + np.cos(np.pi * (np.arange(degree + 1) + 0.5) / (degree + 1)))
    cheb = np.polynomial.Chebyshev.fit(nodes, func(nodes), degree, domain=[0.0, 0.25])
    return [float(v) for v in cheb.convert(kind=np.polynomial.Polynomial).coef]


COS = turn_coefs(lambda u: np.cos(2 * np.pi * np.sqrt(u)), 5)
SIN = turn_coefs(lambda u: np.sin(2 * np.pi * np.sqrt(u)) / np.sqrt(u), 5)


def horner(coefs, u):
    total = jnp.full_like(u, coefs[-1])
    for value in coefs[-2::-1]:
        total = total * u + value
    return total


def turns(product, points, inverse):
    return (product - jnp.round(product * inverse) * points) * inverse


def pad_to(value, unit):
    return -(-value // unit) * unit


def join_lanes(pieces, width):
    lane = lax.broadcasted_iota(jnp.int32, pieces[0].shape, 1)
    total = pad_to(len(pieces) * width, LANES) // LANES
    outs = [None] * total
    for no, piece in enumerate(pieces):
        seat, low = divmod(no * width, LANES)
        moved = pltpu.roll(piece, low, 1) if low else piece
        outs[seat] = moved if low == 0 else jnp.where(lane >= low, moved, outs[seat])
        if low + width > LANES:
            outs[seat + 1] = moved
    return jnp.concatenate(outs, axis=1)


def take_lanes(block, no, width):
    seat, low = divmod(no * width, LANES)
    piece = block[:, seat * LANES : (seat + 1) * LANES]
    if low + width > LANES:
        lane = lax.broadcasted_iota(jnp.int32, piece.shape, 1)
        piece = jnp.where(lane >= low, piece, block[:, (seat + 1) * LANES : (seat + 2) * LANES])
    return pltpu.roll(piece, LANES - low, 1) if low else piece


def trip_kernel(
    chunk,
    stride,
    all_ids,
    all_lengths,
    all_points,
    spec_hbm,
    leg_hbm,
    coef_hbm,
    weight_row,
    in_modes_ref,
    out_modes_ref,
    depth_row,
    update_ref,
    spec_ref,
    leg_ref,
    coef_ref,
    both_ref,
    sent_ref,
    land_ref,
    leave_ref,
    all_ref,
    in_ref,
    out_ref,
    turned_ref,
    give_ref,
    weight_ref,
    depth_ref,
    spec_sem,
    leg_sems,
    coef_sem,
    in_send,
    in_recv,
    out_send,
    out_recv,
    far_send,
    far_recv,
    near_send,
    near_recv,
    own_sems,
    give_send,
    give_recv,
):
    shards, band, lanes = sent_ref.shape
    levs = all_ref.shape[0]
    local_waves, channels, items, span = spec_ref.shape
    half_lat = leg_ref.shape[1]
    half = shards // 2
    fields = channels // 2
    both_rows = channels * items
    rows = both_rows // 2
    padded = both_ref.shape[1] // 2
    waves = shards * local_waves
    lon_max = coef_ref.shape[1]
    chunks = lon_max // LOW
    steps = pad_to(chunks, 8)
    wide = 4 * waves
    modes = in_modes_ref.shape[0]
    parts = band // chunk
    chips = levs // 2
    me = lax.axis_index("wave")
    lev = lax.axis_index("lev")
    reverse = (me * 2) // shards
    chip, core = lev // 2, lax.rem(lev, 2)
    partner = chip * 2 + 1 - core
    peers = [lax.rem(chip + d, chips) * 2 + core for d in range(1, chips)]

    spec_copy = pltpu.make_async_copy(spec_hbm, spec_ref, spec_sem)
    coef_copy = pltpu.make_async_copy(coef_hbm, coef_ref, coef_sem)

    def leg_copy(step, k):
        where = pl.ds(pl.multiple_of(k * band + step * stride, 8), stride)
        return pltpu.make_async_copy(
            leg_hbm.at[:, where, :], leg_ref.at[:, where, :], leg_sems.at[step, k]
        )

    spec_copy.start()

    def start_leg(step, carry):
        for k in range(half):
            leg_copy(step, k).start()
        return carry

    lax.fori_loop(0, band // stride, start_leg, 0)
    coef_copy.start()

    barrier = pltpu.get_barrier_semaphore()
    for away in range(1, shards):
        pl.semaphore_signal(
            barrier,
            inc=1,
            device_id={"wave": lax.rem(me + away, shards)},
            device_id_type=pl.DeviceIdType.MESH,
        )
    for peer in peers + [partner]:
        pl.semaphore_signal(
            barrier, inc=1, device_id={"lev": peer}, device_id_type=pl.DeviceIdType.MESH
        )

    def span_of(part):
        return pl.ds(pl.multiple_of(part * chunk, chunk), chunk)

    def remote(src, dst, send, recv, away, part):
        to = lax.rem(me + away, shards)
        return pltpu.make_async_remote_copy(
            src_ref=src.at[to, span_of(part), :],
            dst_ref=dst.at[me, span_of(part), :],
            send_sem=send.at[away - 1, part],
            recv_sem=recv.at[away - 1, part],
            device_id={"wave": to},
            device_id_type=pl.DeviceIdType.MESH,
        )

    def own(src, dst, which, part):
        return pltpu.make_async_copy(
            src.at[me, span_of(part), :],
            dst.at[me, span_of(part), :],
            own_sems.at[which, part],
        )

    back_ref = all_ref.at[lev]

    def far(away, part):
        return pltpu.make_async_remote_copy(
            src_ref=all_ref.at[lev, :, span_of(part), :],
            dst_ref=all_ref.at[lev, :, span_of(part), :],
            send_sem=far_send.at[away - 1, part],
            recv_sem=far_recv.at[away - 1, part],
            device_id={"lev": peers[away - 1]},
            device_id_type=pl.DeviceIdType.MESH,
        )

    def near(away, part):
        owner = lax.rem(chip + chips - away, chips) * 2 + core
        return pltpu.make_async_remote_copy(
            src_ref=all_ref.at[owner, :, span_of(part), :],
            dst_ref=all_ref.at[owner, :, span_of(part), :],
            send_sem=near_send.at[away, part],
            recv_sem=near_recv.at[away, part],
            device_id={"lev": partner},
            device_id_type=pl.DeviceIdType.MESH,
        )

    def pass_far(part):
        for away in range(1, shards):
            remote(leave_ref, back_ref, out_send, out_recv, away, part).wait_recv()
        own(leave_ref, back_ref, 1, part).wait()
        for away in range(1, chips):
            far(away, part).start()
        near(0, part).start()

    def pass_near(part):
        for away in range(1, chips):
            far(away, part).wait_recv()
            near(away, part).start()

    def start_in(part, carry):
        for away in range(1, shards):
            remote(sent_ref, land_ref, in_send, in_recv, away, part).start()
        own(sent_ref, land_ref, 0, part).start()
        return carry

    spec_copy.wait()
    for m in range(local_waves):
        coeffs = spec_ref[m].reshape(both_rows, span)
        seat = lax.broadcasted_iota(jnp.int32, (both_rows, span), 1)
        live = jnp.where(seat < all_lengths[me * local_waves + m], coeffs.astype(F32), 0.0)
        sign = jnp.where(seat % 2 == 0, live, -live).astype(BF16)
        fill = jnp.zeros((padded - both_rows, span), BF16)
        both_ref[m] = jnp.concatenate([live.astype(BF16), fill, sign, fill], axis=0)

    def inverse(step):
        for k in range(half):
            leg_copy(step, k).wait()
        north, south = [], []
        for m in range(local_waves):
            polys = jnp.concatenate(
                [
                    leg_ref[m, pl.ds(pl.multiple_of(k * band + step * stride, 8), stride), :]
                    for k in range(half)
                ],
                axis=0,
            )
            sums = lax.dot_general(polys, both_ref[m], NTD, preferred_element_type=F32)
            north.append(sums[:, :padded])
            south.append(sums[:, padded:])
        north = join_lanes(north, both_rows).astype(BF16)
        south = join_lanes(south, both_rows).astype(BF16)
        where = pl.ds(pl.multiple_of(step * stride, 8), stride)
        for k in range(half):
            sent_ref[k, where, :] = north[k * stride : (k + 1) * stride]
            sent_ref[shards - 1 - k, where, :] = south[k * stride : (k + 1) * stride]

    each = stride // chunk

    def more(step, carry):
        inverse(step)

        @pl.when(step == 0)
        def _():
            pl.semaphore_wait(barrier, shards - 1 + chips)

        for e in range(each):

            @pl.when(step * each + e < LEAD)
            def _():
                start_in(step * each + e, 0)

        return carry

    lax.fori_loop(0, band // stride, more, 0)
    coef_copy.wait()
    for v in range(weight_row.shape[0]):
        row = weight_row[v : v + 1, :]
        weight_ref[v * LANES : (v + 1) * LANES, :] = jnp.broadcast_to(row, (LANES, LANES)).T
    depth_ref[...] = jnp.broadcast_to(depth_row[...], (LANES, modes)).T

    lane = lax.broadcasted_iota(jnp.int32, (1, wide), 1)
    slot = lane % waves
    wave_lane = jnp.zeros((1, wide), F32)
    columns = []
    for w in range(local_waves):
        for s in range(shards):
            value = all_ids[s * local_waves + w].astype(F32)
            wave_lane = jnp.where(slot == w * shards + s, value, wave_lane)
            columns.append(jnp.full((1, LANES), value, F32))
    wave_col = jnp.concatenate(columns, axis=0)
    quarter = jnp.where(lane < 2 * waves, 0.0, 0.25)
    all_signs = jnp.where(lane < waves, 1.0, -1.0)
    factor = jnp.where(wave_lane == 0.0, 1.0, 2.0)
    step_no = lax.broadcasted_iota(jnp.int32, (steps, wide), 0).astype(F32)
    step_wave = step_no * (wave_lane * float(LOW))
    low_no = lax.broadcasted_iota(jnp.int32, (waves, LANES), 1)
    low_wave = low_no.astype(F32) * wave_col
    row_lane = lax.broadcasted_iota(jnp.int32, (waves, LANES), 1)
    out_lane = lax.broadcasted_iota(jnp.int32, (rows, 2 * waves), 1)
    place = lax.broadcasted_iota(jnp.int32, (1, LOW), 1).astype(F32)
    pick_row = lax.broadcasted_iota(jnp.int32, (rows, LANES), 0)
    pick_lane = lax.broadcasted_iota(jnp.int32, (rows, LANES), 1)
    picks = ((pick_lane == pick_row) | (pick_lane == pick_row + rows)).astype(F32).astype(BF16)
    merge_row = lax.broadcasted_iota(jnp.int32, (waves, 2 * waves), 0)
    merge_lane = lax.broadcasted_iota(jnp.int32, (waves, 2 * waves), 1)
    merges = (merge_lane % waves == merge_row).astype(F32).astype(BF16)

    def prepare(local):
        count = all_points[me * band + local].astype(F32)
        pts = jnp.full((1, wide), count, F32)
        inv = 1.0 / pts
        step = turns(step_wave, pts, inv) - quarter
        step = step - jnp.round(step)
        signs = jnp.where(2.0 * wave_lane < count, all_signs, 0.0)
        anal = horner(COS, step * step) * signs
        synth = anal * factor
        turn = turns(low_wave, pts[:, :LANES], inv[:, :LANES])
        square = turn * turn
        cos_low = horner(COS, square)
        sin_low = horner(SIN, square) * turn
        mid = LANES // 2
        cos_half = jnp.broadcast_to(cos_low[:, mid : mid + 1], cos_low.shape)
        sin_half = jnp.broadcast_to(sin_low[:, mid : mid + 1], sin_low.shape)
        twice = cos_half + cos_half
        cos_full = twice * cos_half - 1.0
        sin_full = twice * sin_half
        cos_far = cos_low * cos_full - sin_low * sin_full
        sin_far = sin_low * cos_full + cos_low * sin_full
        cos_all = jnp.concatenate([cos_low.astype(BF16), cos_far.astype(BF16)], axis=1)
        sin_all = jnp.concatenate([sin_low.astype(BF16), sin_far.astype(BF16)], axis=1)
        return count, inv[:, : 2 * waves], synth, anal, cos_all, sin_all

    def pick(seat):
        data = jnp.concatenate(
            [in_ref[w, pl.ds(seat, shards, stride=chunk), :] for w in range(local_waves)], axis=0
        )
        real = jnp.where(row_lane < rows, data, 0.0).astype(BF16)
        other = (row_lane >= rows) & (row_lane < both_rows)
        imag = jnp.where(other, data, 0.0).astype(BF16)
        four = jnp.concatenate([real, imag, imag, real], axis=0)
        spread = lax.dot_general(picks, four, NTD, preferred_element_type=F32)
        return spread.astype(BF16)

    def tendency(grid, local, pts):
        pieces = []
        for k in range(chunks):
            vals = grid[k * rows : (k + 1) * rows].astype(BF16)
            after = jnp.concatenate([vals[items:], vals[:items]], axis=0)
            coef = coef_ref[pl.ds(local, 1), k * LOW : (k + 1) * LOW]
            coef = jnp.broadcast_to(coef, (items, LOW)).astype(BF16)
            coef = jnp.concatenate([coef] * fields, axis=0)
            tend = vals * (coef + after)
            live = jnp.broadcast_to(place < pts - float(k * LOW), tend.shape)
            pieces.append(jnp.where(live, tend, jnp.zeros_like(tend)))
        return jnp.concatenate(pieces, axis=0)

    def reduce(back, anal, inv):
        total = back[:rows] * anal[0:1, :]
        for k in range(1, chunks):
            total = total + back[k * rows : (k + 1) * rows] * anal[k : k + 1, :]
        result = (total[:, : 2 * waves] + total[:, 2 * waves :]) * inv
        return jnp.concatenate(
            [
                jnp.where(out_lane < waves, result, 0.0).astype(BF16),
                jnp.where(out_lane < waves, 0.0, result).astype(BF16),
                jnp.zeros((LANES - both_rows, 2 * waves), BF16),
            ],
            axis=0,
        )

    def stretch(row):
        block = jnp.broadcast_to(row, (items, wide)).astype(BF16)
        return jnp.concatenate([block] * fields, axis=0)

    def several(part, step, carry):
        seats = [step * GROUP + g for g in range(GROUP)]
        stored = [part * chunk + v for v in seats]
        locals_ = [v + reverse * (band - 1 - 2 * v) for v in stored]
        made = [prepare(v) for v in locals_]
        spreads = [pick(v) for v in seats]
        turned = [
            jnp.concatenate([x * stretch(w[2][k : k + 1, :]) for k in range(chunks)], axis=0)
            for x, w in zip(spreads, made)
        ]
        grids = [
            lax.dot_general(
                x,
                jnp.concatenate([w[4], w[5], w[4], w[5]], axis=0),
                NN,
                preferred_element_type=F32,
            )
            for x, w in zip(turned, made)
        ]
        tends = [tendency(x, v, w[0]) for x, v, w in zip(grids, locals_, made)]
        backs = [
            lax.dot_general(
                x,
                jnp.concatenate([w[4], w[5], w[5], w[4]], axis=0),
                NTD,
                preferred_element_type=F32,
            )
            for x, w in zip(tends, made)
        ]
        splits = [reduce(x, w[3], w[1]) for x, w in zip(backs, made)]
        outs = [lax.dot_general(merges, x, NTD, preferred_element_type=F32) for x in splits]
        for seat, value in zip(seats, outs):
            for w in range(local_waves):
                out_ref[w, pl.ds(seat, shards, stride=chunk), :] = value[
                    w * shards : (w + 1) * shards
                ]
        return carry

    def work(part, carry):
        @pl.when(part + LEAD < parts)
        def _():
            start_in(part + LEAD, 0)

        for away in range(1, shards):
            remote(sent_ref, land_ref, in_send, in_recv, away, part).wait_recv()
        own(sent_ref, land_ref, 0, part).wait()

        @pl.when(part >= FIRST)
        def _():
            pass_far(part - FIRST)

        @pl.when(part >= SECOND)
        def _():
            pass_near(part - SECOND)

        got = land_ref[:, span_of(part), :].astype(F32).reshape(shards * chunk, -1)
        for w in range(local_waves):
            in_ref[w] = take_lanes(got, w, both_rows)
        lax.fori_loop(0, chunk // GROUP, functools.partial(several, part), 0)
        made = join_lanes([out_ref[w] for w in range(local_waves)], both_rows).astype(BF16)
        leave_ref[:, span_of(part), :] = made.reshape(shards, chunk, -1)
        for away in range(1, shards):
            remote(leave_ref, back_ref, out_send, out_recv, away, part).start()
        own(leave_ref, back_ref, 1, part).start()
        return carry

    lax.fori_loop(0, parts, work, 0)

    def rest_far(part, carry):
        pass_far(part)
        return carry

    def rest_near(part, carry):
        pass_near(part)
        return carry

    def landed(part, carry):
        for away in range(chips):
            near(away, part).wait_recv()
        return carry

    lax.fori_loop(max(parts - FIRST, 0), parts, rest_far, 0)
    lax.fori_loop(max(parts - SECOND, 0), parts, rest_near, 0)
    lax.fori_loop(0, parts, landed, 0)

    part_span = span // 2
    start = pl.multiple_of(core * part_span, part_span)
    weights = weight_ref[:half_lat, :1]

    def give(m):
        return pltpu.make_async_remote_copy(
            src_ref=give_ref.at[m],
            dst_ref=update_ref.at[m, :, :, pl.ds(start, part_span)],
            send_sem=give_send.at[m],
            recv_sem=give_recv.at[m],
            device_id={"lev": partner},
            device_id_type=pl.DeviceIdType.MESH,
        )

    def fold(s, carry):
        for v in range(lanes // LANES):
            lane = slice(v * LANES, (v + 1) * LANES)
            north = jnp.concatenate([all_ref[s, k, :, lane] for k in range(half)], axis=0)
            south = jnp.concatenate(
                [all_ref[s, shards - 1 - k, :, lane] for k in range(half)], axis=0
            )
            north = north.astype(F32)
            south = south.astype(F32)
            even = (weights * (north + south)).astype(BF16)
            odd = (weights * (north - south)).astype(BF16)
            turned_ref[s, lane, :half_lat] = even.T
            turned_ref[s, lane, half_lat:] = odd.T
        return carry

    lax.fori_loop(0, levs, fold, 0)
    pair_rows = jnp.concatenate(
        [
            out_modes_ref[pl.ds(pl.multiple_of(r * items, items), items), :]
            for r in (lev, partner)
        ],
        axis=0,
    )

    def one(m, carry):
        seat = lax.broadcasted_iota(jnp.int32, (1, part_span), 1) + start
        leg = leg_ref[m, :, pl.ds(start, part_span)]
        kept = jnp.broadcast_to(seat % 2 == 0, leg.shape)
        none = jnp.zeros_like(leg)
        polys = jnp.concatenate([jnp.where(kept, leg, none), jnp.where(kept, none, leg)], axis=0)
        mine = pl.ds(pl.multiple_of(m * both_rows, both_rows), both_rows)
        pieces = jnp.concatenate([turned_ref[s, mine, :] for s in range(levs)], axis=0)
        values = lax.dot_general(pieces, polys, NN, preferred_element_type=F32)
        values = jnp.where(seat < all_lengths[me * local_waves + m], values, 0.0).astype(BF16)
        degree = (seat + all_ids[me * local_waves + m]).astype(F32)
        damp = 1.0 / (1.0 + depth_ref[:, :1] * degree * (degree + 1.0) / float(NT * NT))
        for c in range(channels):
            stack = jnp.concatenate(
                [
                    values[s * both_rows + c * items : s * both_rows + (c + 1) * items]
                    for s in range(levs)
                ],
                axis=0,
            )
            vals = lax.dot_general(in_modes_ref[...], stack, NN, preferred_element_type=F32)
            scaled = (vals * damp).astype(BF16)
            mixed = lax.dot_general(pair_rows, scaled, NN, preferred_element_type=F32)
            mixed = mixed.astype(BF16)
            update_ref[m, c, :, pl.ds(start, part_span)] = mixed[:items]
            give_ref[m, c] = mixed[items:]
        give(m).start()
        return carry

    lax.fori_loop(0, local_waves, one, 0)

    def finish(part, carry):
        for away in range(1, shards):
            remote(sent_ref, land_ref, in_send, in_recv, away, part).wait_send()
            remote(leave_ref, back_ref, out_send, out_recv, away, part).wait_send()
        for away in range(1, chips):
            far(away, part).wait_send()
        for away in range(chips):
            near(away, part).wait_send()
        return carry

    lax.fori_loop(0, parts, finish, 0)

    def given(m, carry):
        give(m).wait()
        return carry

    lax.fori_loop(0, local_waves, given, 0)


def on_device(
    spectral,
    legendre,
    wave_ids,
    trunc_lengths,
    cycle_points,
    grid_coef,
    cycle_weights,
    modes_in,
    modes_out,
    depths,
):
    shards = lax.axis_size("wave")
    levs = lax.axis_size("lev")
    chips = levs // 2
    waves, channels, items, span = spectral.shape
    half_lat = legendre.shape[1]
    rows = channels * items
    band = grid_coef.shape[0]
    modes = modes_in.shape[0]
    lanes = pad_to(waves * rows, LANES)
    chunk = next(c for c in (16, 8) if band % c == 0)
    stride = next(c * chunk for c in (2, 1) if band % (c * chunk) == 0)
    parts = band // chunk
    messages = (shards, band, lanes)
    vmem = pl.BlockSpec(memory_space=pltpu.VMEM)
    smem = pl.BlockSpec(memory_space=pltpu.SMEM)
    hbm = pl.BlockSpec(memory_space=pltpu.HBM)
    dma = pltpu.SemaphoreType.DMA
    return pl.pallas_call(
        functools.partial(trip_kernel, chunk, stride),
        name="trip",
        out_shape=jax.ShapeDtypeStruct(spectral.shape, BF16),
        in_specs=[smem] * 3 + [hbm] * 3 + [vmem] * 4,
        out_specs=vmem,
        scratch_shapes=[
            pltpu.VMEM(spectral.shape, BF16),
            pltpu.VMEM(legendre.shape, BF16),
            pltpu.VMEM(grid_coef.shape, F32),
            pltpu.VMEM((waves, 2 * pad_to(rows, LANES), span), BF16),
            pltpu.VMEM(messages, BF16),
            pltpu.VMEM(messages, BF16),
            pltpu.VMEM(messages, BF16),
            pltpu.VMEM((levs, *messages), BF16),
            pltpu.VMEM((waves, shards * chunk, LANES), F32),
            pltpu.VMEM((waves, shards * chunk, LANES), F32),
            pltpu.VMEM((levs, lanes, 2 * half_lat), BF16),
            pltpu.VMEM((waves, channels, items, span // 2), BF16),
            pltpu.VMEM((pad_to(half_lat, LANES), LANES), F32),
            pltpu.VMEM((modes, LANES), F32),
            dma,
            dma((band // stride, shards // 2)),
            dma,
            dma((shards - 1, parts)),
            dma((shards - 1, parts)),
            dma((shards - 1, parts)),
            dma((shards - 1, parts)),
            dma((max(chips - 1, 1), parts)),
            dma((max(chips - 1, 1), parts)),
            dma((chips, parts)),
            dma((chips, parts)),
            dma((2, parts)),
            dma((waves,)),
            dma((waves,)),
        ],
        compiler_params=pltpu.CompilerParams(
            vmem_limit_bytes=56 << 20, collective_id=0, has_side_effects=True
        ),
    )(
        wave_ids,
        trunc_lengths,
        cycle_points,
        spectral,
        legendre,
        grid_coef,
        jnp.pad(cycle_weights, (0, -half_lat % LANES)).reshape(-1, LANES),
        modes_in,
        modes_out,
        depths[None, :],
    )


def solution(mesh):
    placed = (
        P("wave", None, "lev", None),
        P("wave", None, None),
        P(),
        P(),
        P(),
        P("wave", None),
        P(),
        P(),
        P(),
        P(),
    )
    return jax.shard_map(
        on_device,
        mesh=mesh,
        in_specs=placed,
        out_specs=P("wave", None, "lev", None),
        check_vma=False,
    )
```

```python
import functools

import jax
import jax.numpy as jnp
import numpy as np
from jax import lax
from jax.experimental import pallas as pl
from jax.experimental.pallas import tpu as pltpu
from jax.sharding import PartitionSpec as P

NT = 1280
LOW = 256
LANES = 128
GROUP = 8
LEAD = 3
FIRST = 4
SECOND = 6
NN = (((1,), (0,)), ((), ()))
NTD = (((1,), (1,)), ((), ()))
F32 = jnp.float32
BF16 = jnp.bfloat16


def turn_coefs(func, degree):
    nodes = 0.125 * (1.0 + np.cos(np.pi * (np.arange(degree + 1) + 0.5) / (degree + 1)))
    cheb = np.polynomial.Chebyshev.fit(nodes, func(nodes), degree, domain=[0.0, 0.25])
    return [float(v) for v in cheb.convert(kind=np.polynomial.Polynomial).coef]


COS = turn_coefs(lambda u: np.cos(2 * np.pi * np.sqrt(u)), 5)
SIN = turn_coefs(lambda u: np.sin(2 * np.pi * np.sqrt(u)) / np.sqrt(u), 5)


def horner(coefs, u):
    total = jnp.full_like(u, coefs[-1])
    for value in coefs[-2::-1]:
        total = total * u + value
    return total


def turns(product, points, inverse):
    return (product - jnp.round(product * inverse) * points) * inverse


def pad_to(value, unit):
    return -(-value // unit) * unit


def join_lanes(pieces, width):
    lane = lax.broadcasted_iota(jnp.int32, pieces[0].shape, 1)
    total = pad_to(len(pieces) * width, LANES) // LANES
    outs = [None] * total
    for no, piece in enumerate(pieces):
        seat, low = divmod(no * width, LANES)
        moved = pltpu.roll(piece, low, 1) if low else piece
        outs[seat] = moved if low == 0 else jnp.where(lane >= low, moved, outs[seat])
        if low + width > LANES:
            outs[seat + 1] = moved
    return jnp.concatenate(outs, axis=1)


def take_lanes(block, no, width):
    seat, low = divmod(no * width, LANES)
    piece = block[:, seat * LANES : (seat + 1) * LANES]
    if low + width > LANES:
        lane = lax.broadcasted_iota(jnp.int32, piece.shape, 1)
        piece = jnp.where(lane >= low, piece, block[:, (seat + 1) * LANES : (seat + 2) * LANES])
    return pltpu.roll(piece, LANES - low, 1) if low else piece


def trip_kernel(
    chunk,
    stride,
    all_ids,
    all_lengths,
    all_points,
    spec_hbm,
    leg_hbm,
    coef_hbm,
    weight_row,
    in_modes_ref,
    out_modes_ref,
    depth_row,
    update_ref,
    spec_ref,
    leg_ref,
    coef_ref,
    both_ref,
    sent_ref,
    land_ref,
    leave_ref,
    all_ref,
    in_ref,
    out_ref,
    turned_ref,
    give_ref,
    weight_ref,
    depth_ref,
    spec_sem,
    leg_sems,
    coef_sem,
    in_send,
    in_recv,
    out_send,
    out_recv,
    far_send,
    far_recv,
    near_send,
    near_recv,
    own_sems,
    give_send,
    give_recv,
):
    shards, band, lanes = sent_ref.shape
    levs = all_ref.shape[0]
    local_waves, channels, items, span = spec_ref.shape
    half_lat = leg_ref.shape[1]
    half = shards // 2
    fields = channels // 2
    both_rows = channels * items
    rows = both_rows // 2
    padded = both_ref.shape[1] // 2
    waves = shards * local_waves
    lon_max = coef_ref.shape[1]
    chunks = lon_max // LOW
    steps = pad_to(chunks, 8)
    wide = 4 * waves
    modes = in_modes_ref.shape[0]
    parts = band // chunk
    chips = levs // 2
    me = lax.axis_index("wave")
    lev = lax.axis_index("lev")
    reverse = (me * 2) // shards
    chip, core = lev // 2, lax.rem(lev, 2)
    partner = chip * 2 + 1 - core
    peers = [lax.rem(chip + d, chips) * 2 + core for d in range(1, chips)]

    spec_copy = pltpu.make_async_copy(spec_hbm, spec_ref, spec_sem)
    coef_copy = pltpu.make_async_copy(coef_hbm, coef_ref, coef_sem)

    def leg_copy(step, k):
        where = pl.ds(pl.multiple_of(k * band + step * stride, 8), stride)
        return pltpu.make_async_copy(
            leg_hbm.at[:, where, :], leg_ref.at[:, where, :], leg_sems.at[step, k]
        )

    spec_copy.start()

    def start_leg(step, carry):
        for k in range(half):
            leg_copy(step, k).start()
        return carry

    lax.fori_loop(0, band // stride, start_leg, 0)
    coef_copy.start()

    barrier = pltpu.get_barrier_semaphore()
    for away in range(1, shards):
        pl.semaphore_signal(
            barrier,
            inc=1,
            device_id={"wave": lax.rem(me + away, shards)},
            device_id_type=pl.DeviceIdType.MESH,
        )
    for peer in peers + [partner]:
        pl.semaphore_signal(
            barrier, inc=1, device_id={"lev": peer}, device_id_type=pl.DeviceIdType.MESH
        )

    def span_of(part):
        return pl.ds(pl.multiple_of(part * chunk, chunk), chunk)

    def remote(src, dst, send, recv, away, part):
        to = lax.rem(me + away, shards)
        return pltpu.make_async_remote_copy(
            src_ref=src.at[to, span_of(part), :],
            dst_ref=dst.at[me, span_of(part), :],
            send_sem=send.at[away - 1, part],
            recv_sem=recv.at[away - 1, part],
            device_id={"wave": to},
            device_id_type=pl.DeviceIdType.MESH,
        )

    def own(src, dst, which, part):
        return pltpu.make_async_copy(
            src.at[me, span_of(part), :],
            dst.at[me, span_of(part), :],
            own_sems.at[which, part],
        )

    back_ref = all_ref.at[lev]

    def far(away, part):
        return pltpu.make_async_remote_copy(
            src_ref=all_ref.at[lev, :, span_of(part), :],
            dst_ref=all_ref.at[lev, :, span_of(part), :],
            send_sem=far_send.at[away - 1, part],
            recv_sem=far_recv.at[away - 1, part],
            device_id={"lev": peers[away - 1]},
            device_id_type=pl.DeviceIdType.MESH,
        )

    def near(away, part):
        owner = lax.rem(chip + chips - away, chips) * 2 + core
        return pltpu.make_async_remote_copy(
            src_ref=all_ref.at[owner, :, span_of(part), :],
            dst_ref=all_ref.at[owner, :, span_of(part), :],
            send_sem=near_send.at[away, part],
            recv_sem=near_recv.at[away, part],
            device_id={"lev": partner},
            device_id_type=pl.DeviceIdType.MESH,
        )

    def pass_far(part):
        for away in range(1, shards):
            remote(leave_ref, back_ref, out_send, out_recv, away, part).wait_recv()
        own(leave_ref, back_ref, 1, part).wait()
        for away in range(1, chips):
            far(away, part).start()
        near(0, part).start()

    def pass_near(part):
        for away in range(1, chips):
            far(away, part).wait_recv()
            near(away, part).start()

    def start_in(part, carry):
        for away in range(1, shards):
            remote(sent_ref, land_ref, in_send, in_recv, away, part).start()
        own(sent_ref, land_ref, 0, part).start()
        return carry

    spec_copy.wait()
    for m in range(local_waves):
        coeffs = spec_ref[m].reshape(both_rows, span)
        seat = lax.broadcasted_iota(jnp.int32, (both_rows, span), 1)
        live = jnp.where(seat < all_lengths[me * local_waves + m], coeffs.astype(F32), 0.0)
        sign = jnp.where(seat % 2 == 0, live, -live).astype(BF16)
        fill = jnp.zeros((padded - both_rows, span), BF16)
        both_ref[m] = jnp.concatenate([live.astype(BF16), fill, sign, fill], axis=0)

    def inverse(step):
        for k in range(half):
            leg_copy(step, k).wait()
        north, south = [], []
        for m in range(local_waves):
            polys = jnp.concatenate(
                [
                    leg_ref[m, pl.ds(pl.multiple_of(k * band + step * stride, 8), stride), :]
                    for k in range(half)
                ],
                axis=0,
            )
            sums = lax.dot_general(polys, both_ref[m], NTD, preferred_element_type=F32)
            north.append(sums[:, :padded])
            south.append(sums[:, padded:])
        north = join_lanes(north, both_rows).astype(BF16)
        south = join_lanes(south, both_rows).astype(BF16)
        where = pl.ds(pl.multiple_of(step * stride, 8), stride)
        for k in range(half):
            sent_ref[k, where, :] = north[k * stride : (k + 1) * stride]
            sent_ref[shards - 1 - k, where, :] = south[k * stride : (k + 1) * stride]

    each = stride // chunk

    def more(step, carry):
        inverse(step)

        @pl.when(step == 0)
        def _():
            pl.semaphore_wait(barrier, shards - 1 + chips)

        for e in range(each):

            @pl.when(step * each + e < LEAD)
            def _():
                start_in(step * each + e, 0)

        return carry

    lax.fori_loop(0, band // stride, more, 0)
    coef_copy.wait()
    for v in range(weight_row.shape[0]):
        row = weight_row[v : v + 1, :]
        weight_ref[v * LANES : (v + 1) * LANES, :] = jnp.broadcast_to(row, (LANES, LANES)).T
    depth_ref[...] = jnp.broadcast_to(depth_row[...], (LANES, modes)).T

    lane = lax.broadcasted_iota(jnp.int32, (1, wide), 1)
    slot = lane % waves
    wave_lane = jnp.zeros((1, wide), F32)
    columns = []
    for w in range(local_waves):
        for s in range(shards):
            value = all_ids[s * local_waves + w].astype(F32)
            wave_lane = jnp.where(slot == w * shards + s, value, wave_lane)
            columns.append(jnp.full((1, LANES), value, F32))
    wave_col = jnp.concatenate(columns, axis=0)
    quarter = jnp.where(lane < 2 * waves, 0.0, 0.25)
    all_signs = jnp.where(lane < waves, 1.0, -1.0)
    factor = jnp.where(wave_lane == 0.0, 1.0, 2.0)
    step_no = lax.broadcasted_iota(jnp.int32, (steps, wide), 0).astype(F32)
    step_wave = step_no * (wave_lane * float(LOW))
    low_no = lax.broadcasted_iota(jnp.int32, (waves, LANES), 1)
    low_wave = low_no.astype(F32) * wave_col
    row_lane = lax.broadcasted_iota(jnp.int32, (waves, LANES), 1)
    out_lane = lax.broadcasted_iota(jnp.int32, (rows, 2 * waves), 1)
    place = lax.broadcasted_iota(jnp.int32, (1, LOW), 1).astype(F32)
    pick_row = lax.broadcasted_iota(jnp.int32, (rows, LANES), 0)
    pick_lane = lax.broadcasted_iota(jnp.int32, (rows, LANES), 1)
    picks = ((pick_lane == pick_row) | (pick_lane == pick_row + rows)).astype(F32).astype(BF16)
    merge_row = lax.broadcasted_iota(jnp.int32, (waves, 2 * waves), 0)
    merge_lane = lax.broadcasted_iota(jnp.int32, (waves, 2 * waves), 1)
    merges = (merge_lane % waves == merge_row).astype(F32).astype(BF16)

    def prepare(local):
        count = all_points[me * band + local].astype(F32)
        pts = jnp.full((1, wide), count, F32)
        inv = 1.0 / pts
        step = turns(step_wave, pts, inv) - quarter
        step = step - jnp.round(step)
        signs = jnp.where(2.0 * wave_lane < count, all_signs, 0.0)
        anal = horner(COS, step * step) * signs
        synth = anal * factor
        turn = turns(low_wave, pts[:, :LANES], inv[:, :LANES])
        square = turn * turn
        cos_low = horner(COS, square)
        sin_low = horner(SIN, square) * turn
        mid = LANES // 2
        cos_half = jnp.broadcast_to(cos_low[:, mid : mid + 1], cos_low.shape)
        sin_half = jnp.broadcast_to(sin_low[:, mid : mid + 1], sin_low.shape)
        twice = cos_half + cos_half
        cos_full = twice * cos_half - 1.0
        sin_full = twice * sin_half
        cos_far = cos_low * cos_full - sin_low * sin_full
        sin_far = sin_low * cos_full + cos_low * sin_full
        cos_all = jnp.concatenate([cos_low.astype(BF16), cos_far.astype(BF16)], axis=1)
        sin_all = jnp.concatenate([sin_low.astype(BF16), sin_far.astype(BF16)], axis=1)
        return count, inv[:, : 2 * waves], synth, anal, cos_all, sin_all

    def pick(seat):
        data = jnp.concatenate(
            [in_ref[w, pl.ds(seat, shards, stride=chunk), :] for w in range(local_waves)], axis=0
        )
        real = jnp.where(row_lane < rows, data, 0.0).astype(BF16)
        other = (row_lane >= rows) & (row_lane < both_rows)
        imag = jnp.where(other, data, 0.0).astype(BF16)
        four = jnp.concatenate([real, imag, imag, real], axis=0)
        spread = lax.dot_general(picks, four, NTD, preferred_element_type=F32)
        return spread.astype(BF16)

    def tendency(grid, local, pts):
        pieces = []
        for k in range(chunks):
            vals = grid[k * rows : (k + 1) * rows].astype(BF16)
            after = jnp.concatenate([vals[items:], vals[:items]], axis=0)
            coef = coef_ref[pl.ds(local, 1), k * LOW : (k + 1) * LOW]
            coef = jnp.broadcast_to(coef, (items, LOW)).astype(BF16)
            coef = jnp.concatenate([coef] * fields, axis=0)
            tend = vals * (coef + after)
            live = jnp.broadcast_to(place < pts - float(k * LOW), tend.shape)
            pieces.append(jnp.where(live, tend, jnp.zeros_like(tend)))
        return jnp.concatenate(pieces, axis=0)

    def reduce(back, anal, inv):
        total = back[:rows] * anal[0:1, :]
        for k in range(1, chunks):
            total = total + back[k * rows : (k + 1) * rows] * anal[k : k + 1, :]
        result = (total[:, : 2 * waves] + total[:, 2 * waves :]) * inv
        return jnp.concatenate(
            [
                jnp.where(out_lane < waves, result, 0.0).astype(BF16),
                jnp.where(out_lane < waves, 0.0, result).astype(BF16),
                jnp.zeros((LANES - both_rows, 2 * waves), BF16),
            ],
            axis=0,
        )

    def stretch(row):
        block = jnp.broadcast_to(row, (items, wide)).astype(BF16)
        return jnp.concatenate([block] * fields, axis=0)

    def several(part, step, carry):
        seats = [step * GROUP + g for g in range(GROUP)]
        stored = [part * chunk + v for v in seats]
        locals_ = [v + reverse * (band - 1 - 2 * v) for v in stored]
        made = [prepare(v) for v in locals_]
        spreads = [pick(v) for v in seats]
        turned = [
            jnp.concatenate([x * stretch(w[2][k : k + 1, :]) for k in range(chunks)], axis=0)
            for x, w in zip(spreads, made)
        ]
        grids = [
            lax.dot_general(
                x,
                jnp.concatenate([w[4], w[5], w[4], w[5]], axis=0),
                NN,
                preferred_element_type=F32,
            )
            for x, w in zip(turned, made)
        ]
        tends = [tendency(x, v, w[0]) for x, v, w in zip(grids, locals_, made)]
        backs = [
            lax.dot_general(
                x,
                jnp.concatenate([w[4], w[5], w[5], w[4]], axis=0),
                NTD,
                preferred_element_type=F32,
            )
            for x, w in zip(tends, made)
        ]
        splits = [reduce(x, w[3], w[1]) for x, w in zip(backs, made)]
        outs = [lax.dot_general(merges, x, NTD, preferred_element_type=F32) for x in splits]
        for seat, value in zip(seats, outs):
            for w in range(local_waves):
                out_ref[w, pl.ds(seat, shards, stride=chunk), :] = value[
                    w * shards : (w + 1) * shards
                ]
        return carry

    def work(part, carry):
        @pl.when(part + LEAD < parts)
        def _():
            start_in(part + LEAD, 0)

        for away in range(1, shards):
            remote(sent_ref, land_ref, in_send, in_recv, away, part).wait_recv()
        own(sent_ref, land_ref, 0, part).wait()

        @pl.when(part >= FIRST)
        def _():
            pass_far(part - FIRST)

        @pl.when(part >= SECOND)
        def _():
            pass_near(part - SECOND)

        got = land_ref[:, span_of(part), :].astype(F32).reshape(shards * chunk, -1)
        for w in range(local_waves):
            in_ref[w] = take_lanes(got, w, both_rows)
        lax.fori_loop(0, chunk // GROUP, functools.partial(several, part), 0)
        made = join_lanes([out_ref[w] for w in range(local_waves)], both_rows).astype(BF16)
        leave_ref[:, span_of(part), :] = made.reshape(shards, chunk, -1)
        for away in range(1, shards):
            remote(leave_ref, back_ref, out_send, out_recv, away, part).start()
        own(leave_ref, back_ref, 1, part).start()
        return carry

    lax.fori_loop(0, parts, work, 0)

    part_span = span // 2
    start = pl.multiple_of(core * part_span, part_span)
    def give(m):
        return pltpu.make_async_remote_copy(
            src_ref=give_ref.at[m],
            dst_ref=update_ref.at[m, :, :, pl.ds(start, part_span)],
            send_sem=give_send.at[m],
            recv_sem=give_recv.at[m],
            device_id={"lev": partner},
            device_id_type=pl.DeviceIdType.MESH,
        )

    def fold(part, carry):
        for away in range(chips):
            near(away, part).wait_recv()
        weights = jnp.concatenate(
            [
                weight_ref[pl.ds(pl.multiple_of(k * band + part * chunk, 8), chunk), :]
                for k in range(half)
            ],
            axis=0,
        )
        sides = []
        for s in range(levs):
            pieces = []
            for v in range(lanes // LANES):
                lane = slice(v * LANES, (v + 1) * LANES)
                north, south = [
                    jnp.concatenate([all_ref[s, k, span_of(part), lane] for k in order], axis=0)
                    for order in (range(half), [shards - 1 - k for k in range(half)])
                ]
                north = north.astype(F32)
                south = south.astype(F32)
                even = (weights * (north + south)).astype(BF16)
                odd = (weights * (north - south)).astype(BF16)
                pieces.append(jnp.concatenate([even, odd], axis=0).T)
            sides.append(jnp.concatenate(pieces, axis=0))
        for m in range(local_waves):
            for c in range(channels):
                low = m * both_rows + c * items
                stack = jnp.concatenate([side[low : low + items] for side in sides], axis=0)
                vals = lax.dot_general(in_modes_ref[...], stack, NN, preferred_element_type=F32)
                turned_ref[part, m, c * modes : (c + 1) * modes, :] = vals.astype(BF16)
        return carry

    def ready(turn):
        return jnp.clip(jnp.minimum(2 * (turn + 1), parts - SECOND + turn), 0, parts)

    def drain(turn, carry):
        @pl.when((parts - FIRST + turn >= 0) & (turn < FIRST))
        def _():
            pass_far(parts - FIRST + turn)

        @pl.when((parts - SECOND + turn >= 0) & (turn < SECOND))
        def _():
            pass_near(parts - SECOND + turn)

        lax.fori_loop(ready(turn - 1), ready(turn), fold, 0)
        return carry

    lax.fori_loop(0, max(SECOND, -(-parts // 2) - 1) + 1, drain, 0)
    pair_rows = jnp.concatenate(
        [
            out_modes_ref[pl.ds(pl.multiple_of(r * items, items), items), :]
            for r in (lev, partner)
        ],
        axis=0,
    )

    def one(m, carry):
        seat = lax.broadcasted_iota(jnp.int32, (1, part_span), 1) + start
        polys = []
        for p in range(parts):
            leg = jnp.concatenate(
                [
                    leg_ref[m, k * band + p * chunk : k * band + (p + 1) * chunk, pl.ds(start, part_span)]
                    for k in range(half)
                ],
                axis=0,
            )
            kept = jnp.broadcast_to(seat % 2 == 0, leg.shape)
            none = jnp.zeros_like(leg)
            polys += [jnp.where(kept, leg, none), jnp.where(kept, none, leg)]
        values = lax.dot_general(
            jnp.concatenate([turned_ref[p, m] for p in range(parts)], axis=1),
            jnp.concatenate(polys, axis=0),
            NN,
            preferred_element_type=F32,
        )
        degree = (seat + all_ids[me * local_waves + m]).astype(F32)
        live = seat < all_lengths[me * local_waves + m]
        damp = 1.0 / (1.0 + depth_ref[:, :1] * degree * (degree + 1.0) / float(NT * NT))
        damp = jnp.where(live, damp, 0.0)
        for c in range(channels):
            scaled = (values[c * modes : (c + 1) * modes] * damp).astype(BF16)
            mixed = lax.dot_general(pair_rows, scaled, NN, preferred_element_type=F32)
            mixed = mixed.astype(BF16)
            update_ref[m, c, :, pl.ds(start, part_span)] = mixed[:items]
            give_ref[m, c] = mixed[items:]
        give(m).start()
        return carry

    lax.fori_loop(0, local_waves, one, 0)

    def finish(part, carry):
        for away in range(1, shards):
            remote(sent_ref, land_ref, in_send, in_recv, away, part).wait_send()
            remote(leave_ref, back_ref, out_send, out_recv, away, part).wait_send()
        for away in range(1, chips):
            far(away, part).wait_send()
        for away in range(chips):
            near(away, part).wait_send()
        return carry

    lax.fori_loop(0, parts, finish, 0)

    def given(m, carry):
        give(m).wait()
        return carry

    lax.fori_loop(0, local_waves, given, 0)


def on_device(
    spectral,
    legendre,
    wave_ids,
    trunc_lengths,
    cycle_points,
    grid_coef,
    cycle_weights,
    modes_in,
    modes_out,
    depths,
):
    shards = lax.axis_size("wave")
    levs = lax.axis_size("lev")
    chips = levs // 2
    waves, channels, items, span = spectral.shape
    half_lat = legendre.shape[1]
    rows = channels * items
    band = grid_coef.shape[0]
    modes = modes_in.shape[0]
    lanes = pad_to(waves * rows, LANES)
    chunk = next(c for c in (16, 8) if band % c == 0)
    stride = next(c * chunk for c in (2, 1) if band % (c * chunk) == 0)
    parts = band // chunk
    messages = (shards, band, lanes)
    vmem = pl.BlockSpec(memory_space=pltpu.VMEM)
    smem = pl.BlockSpec(memory_space=pltpu.SMEM)
    hbm = pl.BlockSpec(memory_space=pltpu.HBM)
    dma = pltpu.SemaphoreType.DMA
    return pl.pallas_call(
        functools.partial(trip_kernel, chunk, stride),
        name="trip",
        out_shape=jax.ShapeDtypeStruct(spectral.shape, BF16),
        in_specs=[smem] * 3 + [hbm] * 3 + [vmem] * 4,
        out_specs=vmem,
        scratch_shapes=[
            pltpu.VMEM(spectral.shape, BF16),
            pltpu.VMEM(legendre.shape, BF16),
            pltpu.VMEM(grid_coef.shape, F32),
            pltpu.VMEM((waves, 2 * pad_to(rows, LANES), span), BF16),
            pltpu.VMEM(messages, BF16),
            pltpu.VMEM(messages, BF16),
            pltpu.VMEM(messages, BF16),
            pltpu.VMEM((levs, *messages), BF16),
            pltpu.VMEM((waves, shards * chunk, LANES), F32),
            pltpu.VMEM((waves, shards * chunk, LANES), F32),
            pltpu.VMEM((parts, waves, channels * modes, shards * chunk), BF16),
            pltpu.VMEM((waves, channels, items, span // 2), BF16),
            pltpu.VMEM((pad_to(half_lat, LANES), LANES), F32),
            pltpu.VMEM((modes, LANES), F32),
            dma,
            dma((band // stride, shards // 2)),
            dma,
            dma((shards - 1, parts)),
            dma((shards - 1, parts)),
            dma((shards - 1, parts)),
            dma((shards - 1, parts)),
            dma((max(chips - 1, 1), parts)),
            dma((max(chips - 1, 1), parts)),
            dma((chips, parts)),
            dma((chips, parts)),
            dma((2, parts)),
            dma((waves,)),
            dma((waves,)),
        ],
        compiler_params=pltpu.CompilerParams(
            vmem_limit_bytes=56 << 20, collective_id=0, has_side_effects=True
        ),
    )(
        wave_ids,
        trunc_lengths,
        cycle_points,
        spectral,
        legendre,
        grid_coef,
        jnp.pad(cycle_weights, (0, -half_lat % LANES)).reshape(-1, LANES),
        modes_in,
        modes_out,
        depths[None, :],
    )


def solution(mesh):
    placed = (
        P("wave", None, "lev", None),
        P("wave", None, None),
        P(),
        P(),
        P(),
        P("wave", None),
        P(),
        P(),
        P(),
        P(),
    )
    return jax.shard_map(
        on_device,
        mesh=mesh,
        in_specs=placed,
        out_specs=P("wave", None, "lev", None),
        check_vma=False,
    )
```

```python
import functools

import jax
import jax.numpy as jnp
import numpy as np
from jax import lax
from jax.experimental import pallas as pl
from jax.experimental.pallas import tpu as pltpu
from jax.sharding import PartitionSpec as P

NT = 1280
LOW = 256
LANES = 128
GROUP = 8
LEAD = 3
FIRST = 4
SECOND = 6
THIRD = 10
NN = (((1,), (0,)), ((), ()))
NTD = (((1,), (1,)), ((), ()))
F32 = jnp.float32
BF16 = jnp.bfloat16


def turn_coefs(func, degree):
    nodes = 0.125 * (1.0 + np.cos(np.pi * (np.arange(degree + 1) + 0.5) / (degree + 1)))
    cheb = np.polynomial.Chebyshev.fit(nodes, func(nodes), degree, domain=[0.0, 0.25])
    return [float(v) for v in cheb.convert(kind=np.polynomial.Polynomial).coef]


COS = turn_coefs(lambda u: np.cos(2 * np.pi * np.sqrt(u)), 5)
SIN = turn_coefs(lambda u: np.sin(2 * np.pi * np.sqrt(u)) / np.sqrt(u), 5)


def horner(coefs, u):
    total = jnp.full_like(u, coefs[-1])
    for value in coefs[-2::-1]:
        total = total * u + value
    return total


def turns(product, points, inverse):
    return (product - jnp.round(product * inverse) * points) * inverse


def pad_to(value, unit):
    return -(-value // unit) * unit


def join_lanes(pieces, width):
    lane = lax.broadcasted_iota(jnp.int32, pieces[0].shape, 1)
    total = pad_to(len(pieces) * width, LANES) // LANES
    outs = [None] * total
    for no, piece in enumerate(pieces):
        seat, low = divmod(no * width, LANES)
        moved = pltpu.roll(piece, low, 1) if low else piece
        outs[seat] = moved if low == 0 else jnp.where(lane >= low, moved, outs[seat])
        if low + width > LANES:
            outs[seat + 1] = moved
    return jnp.concatenate(outs, axis=1)


def take_lanes(block, no, width):
    seat, low = divmod(no * width, LANES)
    piece = block[:, seat * LANES : (seat + 1) * LANES]
    if low + width > LANES:
        lane = lax.broadcasted_iota(jnp.int32, piece.shape, 1)
        piece = jnp.where(lane >= low, piece, block[:, (seat + 1) * LANES : (seat + 2) * LANES])
    return pltpu.roll(piece, LANES - low, 1) if low else piece


def trip_kernel(
    chunk,
    stride,
    all_ids,
    all_lengths,
    all_points,
    spec_hbm,
    leg_hbm,
    coef_hbm,
    weight_row,
    in_modes_ref,
    out_modes_ref,
    depth_row,
    update_ref,
    spec_ref,
    leg_ref,
    coef_ref,
    both_ref,
    sent_ref,
    land_ref,
    leave_ref,
    all_ref,
    in_ref,
    out_ref,
    turned_ref,
    give_ref,
    weight_ref,
    depth_ref,
    acc_ref,
    spec_sem,
    leg_sems,
    coef_sem,
    in_send,
    in_recv,
    out_send,
    out_recv,
    far_send,
    far_recv,
    near_send,
    near_recv,
    own_sems,
    give_send,
    give_recv,
):
    shards, band, lanes = sent_ref.shape
    levs = all_ref.shape[0]
    local_waves, channels, items, span = spec_ref.shape
    half_lat = leg_ref.shape[1]
    half = shards // 2
    fields = channels // 2
    both_rows = channels * items
    rows = both_rows // 2
    padded = both_ref.shape[1] // 2
    waves = shards * local_waves
    lon_max = coef_ref.shape[1]
    chunks = lon_max // LOW
    steps = pad_to(chunks, 8)
    wide = 4 * waves
    modes = in_modes_ref.shape[0]
    parts = band // chunk
    chips = levs // 2
    me = lax.axis_index("wave")
    lev = lax.axis_index("lev")
    reverse = (me * 2) // shards
    chip, core = lev // 2, lax.rem(lev, 2)
    partner = chip * 2 + 1 - core
    peers = [lax.rem(chip + d, chips) * 2 + core for d in range(1, chips)]

    spec_copy = pltpu.make_async_copy(spec_hbm, spec_ref, spec_sem)
    coef_copy = pltpu.make_async_copy(coef_hbm, coef_ref, coef_sem)

    def leg_copy(step, k):
        where = pl.ds(pl.multiple_of(k * band + step * stride, 8), stride)
        return pltpu.make_async_copy(
            leg_hbm.at[:, where, :], leg_ref.at[:, where, :], leg_sems.at[step]
        )

    spec_copy.start()

    def start_leg(step, carry):
        for k in range(half):
            leg_copy(step, k).start()
        return carry

    lax.fori_loop(0, band // stride, start_leg, 0)
    coef_copy.start()

    barrier = pltpu.get_barrier_semaphore()
    for away in range(1, shards):
        pl.semaphore_signal(
            barrier,
            inc=1,
            device_id={"wave": lax.rem(me + away, shards)},
            device_id_type=pl.DeviceIdType.MESH,
        )
    for peer in peers + [partner]:
        pl.semaphore_signal(
            barrier, inc=1, device_id={"lev": peer}, device_id_type=pl.DeviceIdType.MESH
        )

    def span_of(part):
        return pl.ds(pl.multiple_of(part * chunk, chunk), chunk)

    def remote(src, dst, send, recv, away, part):
        to = lax.rem(me + away, shards)
        return pltpu.make_async_remote_copy(
            src_ref=src.at[to, span_of(part), :],
            dst_ref=dst.at[me, span_of(part), :],
            send_sem=send,
            recv_sem=recv.at[part],
            device_id={"wave": to},
            device_id_type=pl.DeviceIdType.MESH,
        )

    def arrived(dst, send, recv, part):
        block = dst.at[pl.ds(0, shards - 1), span_of(part), :]
        return pltpu.make_async_remote_copy(
            src_ref=block,
            dst_ref=block,
            send_sem=send,
            recv_sem=recv.at[part],
            device_id={"wave": lax.rem(me + 1, shards)},
            device_id_type=pl.DeviceIdType.MESH,
        )

    def departed(src, send, recv):
        block = src.at[pl.ds(0, shards - 1)]
        return pltpu.make_async_remote_copy(
            src_ref=block,
            dst_ref=block,
            send_sem=send,
            recv_sem=recv.at[0],
            device_id={"wave": lax.rem(me + 1, shards)},
            device_id_type=pl.DeviceIdType.MESH,
        )

    def own(src, dst, which, part):
        return pltpu.make_async_copy(
            src.at[me, span_of(part), :],
            dst.at[me, span_of(part), :],
            own_sems.at[which, part],
        )

    back_ref = all_ref.at[lev]

    def far(away, part):
        return pltpu.make_async_remote_copy(
            src_ref=all_ref.at[lev, :, span_of(part), :],
            dst_ref=all_ref.at[lev, :, span_of(part), :],
            send_sem=far_send.at[away - 1, part],
            recv_sem=far_recv.at[away - 1, part],
            device_id={"lev": peers[away - 1]},
            device_id_type=pl.DeviceIdType.MESH,
        )

    def near(away, part):
        owner = lax.rem(chip + chips - away, chips) * 2 + core
        return pltpu.make_async_remote_copy(
            src_ref=all_ref.at[owner, :, span_of(part), :],
            dst_ref=all_ref.at[owner, :, span_of(part), :],
            send_sem=near_send.at[away, part],
            recv_sem=near_recv.at[away, part],
            device_id={"lev": partner},
            device_id_type=pl.DeviceIdType.MESH,
        )

    def pass_far(part):
        arrived(back_ref, out_send, out_recv, part).wait_recv()
        own(leave_ref, back_ref, 1, part).wait()
        for away in range(1, chips):
            far(away, part).start()
        near(0, part).start()

    def pass_near(part):
        for away in range(1, chips):
            far(away, part).wait_recv()
            near(away, part).start()

    def start_in(part, carry):
        for away in range(1, shards):
            remote(sent_ref, land_ref, in_send, in_recv, away, part).start()
        own(sent_ref, land_ref, 0, part).start()
        return carry

    spec_copy.wait()
    for m in range(local_waves):
        coeffs = spec_ref[m].reshape(both_rows, span)
        seat = lax.broadcasted_iota(jnp.int32, (both_rows, span), 1)
        live = jnp.where(seat < all_lengths[me * local_waves + m], coeffs.astype(F32), 0.0)
        sign = jnp.where(seat % 2 == 0, live, -live).astype(BF16)
        fill = jnp.zeros((padded - both_rows, span), BF16)
        both_ref[m] = jnp.concatenate([live.astype(BF16), fill, sign, fill], axis=0)

    def inverse(step):
        taken = leg_ref.at[:, pl.ds(0, half * stride), :]
        pltpu.make_async_copy(taken, taken, leg_sems.at[step]).wait()
        north, south = [], []
        for m in range(local_waves):
            polys = jnp.concatenate(
                [
                    leg_ref[m, pl.ds(pl.multiple_of(k * band + step * stride, 8), stride), :]
                    for k in range(half)
                ],
                axis=0,
            )
            sums = lax.dot_general(polys, both_ref[m], NTD, preferred_element_type=F32)
            north.append(sums[:, :padded])
            south.append(sums[:, padded:])
        north = join_lanes(north, both_rows).astype(BF16)
        south = join_lanes(south, both_rows).astype(BF16)
        where = pl.ds(pl.multiple_of(step * stride, 8), stride)
        for k in range(half):
            sent_ref[k, where, :] = north[k * stride : (k + 1) * stride]
            sent_ref[shards - 1 - k, where, :] = south[k * stride : (k + 1) * stride]

    each = stride // chunk

    def more(step, carry):
        inverse(step)

        @pl.when(step == 0)
        def _():
            pl.semaphore_wait(barrier, shards - 1 + chips)

        for e in range(each):

            @pl.when(step * each + e < LEAD)
            def _():
                start_in(step * each + e, 0)

        return carry

    lax.fori_loop(0, band // stride, more, 0)
    coef_copy.wait()
    for v in range(weight_row.shape[0]):
        row = weight_row[v : v + 1, :]
        weight_ref[v * LANES : (v + 1) * LANES, :] = jnp.broadcast_to(row, (LANES, LANES)).T
    depth_ref[...] = jnp.broadcast_to(depth_row[...], (LANES, modes)).T

    lane = lax.broadcasted_iota(jnp.int32, (1, wide), 1)
    slot = lane % waves
    wave_lane = jnp.zeros((1, wide), F32)
    columns = []
    for w in range(local_waves):
        for s in range(shards):
            value = all_ids[s * local_waves + w].astype(F32)
            wave_lane = jnp.where(slot == w * shards + s, value, wave_lane)
            columns.append(jnp.full((1, LANES), value, F32))
    wave_col = jnp.concatenate(columns, axis=0)
    quarter = jnp.where(lane < 2 * waves, 0.0, 0.25)
    all_signs = jnp.where(lane < waves, 1.0, -1.0)
    factor = jnp.where(wave_lane == 0.0, 1.0, 2.0)
    step_no = lax.broadcasted_iota(jnp.int32, (steps, wide), 0).astype(F32)
    step_wave = step_no * (wave_lane * float(LOW))
    low_no = lax.broadcasted_iota(jnp.int32, (waves, LANES), 1)
    low_wave = low_no.astype(F32) * wave_col
    row_lane = lax.broadcasted_iota(jnp.int32, (waves, LANES), 1)
    out_lane = lax.broadcasted_iota(jnp.int32, (rows, 2 * waves), 1)
    place = lax.broadcasted_iota(jnp.int32, (1, LOW), 1).astype(F32)
    pick_row = lax.broadcasted_iota(jnp.int32, (rows, LANES), 0)
    pick_lane = lax.broadcasted_iota(jnp.int32, (rows, LANES), 1)
    picks = ((pick_lane == pick_row) | (pick_lane == pick_row + rows)).astype(F32).astype(BF16)
    merge_row = lax.broadcasted_iota(jnp.int32, (waves, 2 * waves), 0)
    merge_lane = lax.broadcasted_iota(jnp.int32, (waves, 2 * waves), 1)
    merges = (merge_lane % waves == merge_row).astype(F32).astype(BF16)

    def prepare(local):
        count = all_points[me * band + local].astype(F32)
        pts = jnp.full((1, wide), count, F32)
        inv = 1.0 / pts
        step = turns(step_wave, pts, inv) - quarter
        step = step - jnp.round(step)
        signs = jnp.where(2.0 * wave_lane < count, all_signs, 0.0)
        anal = horner(COS, step * step) * signs
        synth = anal * factor
        turn = turns(low_wave, pts[:, :LANES], inv[:, :LANES])
        square = turn * turn
        cos_low = horner(COS, square)
        sin_low = horner(SIN, square) * turn
        mid = LANES // 2
        cos_half = jnp.broadcast_to(cos_low[:, mid : mid + 1], cos_low.shape)
        sin_half = jnp.broadcast_to(sin_low[:, mid : mid + 1], sin_low.shape)
        twice = cos_half + cos_half
        cos_full = twice * cos_half - 1.0
        sin_full = twice * sin_half
        cos_far = cos_low * cos_full - sin_low * sin_full
        sin_far = sin_low * cos_full + cos_low * sin_full
        cos_all = jnp.concatenate([cos_low.astype(BF16), cos_far.astype(BF16)], axis=1)
        sin_all = jnp.concatenate([sin_low.astype(BF16), sin_far.astype(BF16)], axis=1)
        return count, inv[:, : 2 * waves], synth, anal, cos_all, sin_all

    def pick(seat):
        data = jnp.concatenate(
            [in_ref[w, pl.ds(seat, shards, stride=chunk), :] for w in range(local_waves)], axis=0
        )
        real = jnp.where(row_lane < rows, data, 0.0).astype(BF16)
        other = (row_lane >= rows) & (row_lane < both_rows)
        imag = jnp.where(other, data, 0.0).astype(BF16)
        four = jnp.concatenate([real, imag, imag, real], axis=0)
        spread = lax.dot_general(picks, four, NTD, preferred_element_type=F32)
        return spread.astype(BF16)

    def tendency(grid, local, pts):
        pieces = []
        for k in range(chunks):
            vals = grid[k * rows : (k + 1) * rows].astype(BF16)
            after = jnp.concatenate([vals[items:], vals[:items]], axis=0)
            coef = coef_ref[pl.ds(local, 1), k * LOW : (k + 1) * LOW]
            coef = jnp.broadcast_to(coef, (items, LOW)).astype(BF16)
            coef = jnp.concatenate([coef] * fields, axis=0)
            tend = vals * (coef + after)
            live = jnp.broadcast_to(place < pts - float(k * LOW), tend.shape)
            pieces.append(jnp.where(live, tend, jnp.zeros_like(tend)))
        return jnp.concatenate(pieces, axis=0)

    def reduce(back, anal, inv):
        total = back[:rows] * anal[0:1, :]
        for k in range(1, chunks):
            total = total + back[k * rows : (k + 1) * rows] * anal[k : k + 1, :]
        result = (total[:, : 2 * waves] + total[:, 2 * waves :]) * inv
        return jnp.concatenate(
            [
                jnp.where(out_lane < waves, result, 0.0).astype(BF16),
                jnp.where(out_lane < waves, 0.0, result).astype(BF16),
                jnp.zeros((LANES - both_rows, 2 * waves), BF16),
            ],
            axis=0,
        )

    def stretch(row):
        block = jnp.broadcast_to(row, (items, wide)).astype(BF16)
        return jnp.concatenate([block] * fields, axis=0)

    def several(part, step, carry):
        seats = [step * GROUP + g for g in range(GROUP)]
        stored = [part * chunk + v for v in seats]
        locals_ = [v + reverse * (band - 1 - 2 * v) for v in stored]
        made = [prepare(v) for v in locals_]
        spreads = [pick(v) for v in seats]
        turned = [
            jnp.concatenate([x * stretch(w[2][k : k + 1, :]) for k in range(chunks)], axis=0)
            for x, w in zip(spreads, made)
        ]
        grids = [
            lax.dot_general(
                x,
                jnp.concatenate([w[4], w[5], w[4], w[5]], axis=0),
                NN,
                preferred_element_type=F32,
            )
            for x, w in zip(turned, made)
        ]
        tends = [tendency(x, v, w[0]) for x, v, w in zip(grids, locals_, made)]
        backs = [
            lax.dot_general(
                x,
                jnp.concatenate([w[4], w[5], w[5], w[4]], axis=0),
                NTD,
                preferred_element_type=F32,
            )
            for x, w in zip(tends, made)
        ]
        splits = [reduce(x, w[3], w[1]) for x, w in zip(backs, made)]
        outs = [lax.dot_general(merges, x, NTD, preferred_element_type=F32) for x in splits]
        for seat, value in zip(seats, outs):
            for w in range(local_waves):
                out_ref[w, pl.ds(seat, shards, stride=chunk), :] = value[
                    w * shards : (w + 1) * shards
                ]
        return carry

    def fold(part, carry):
        for away in range(chips):
            near(away, part).wait_recv()
        weights = jnp.concatenate(
            [
                weight_ref[pl.ds(pl.multiple_of(k * band + part * chunk, 8), chunk), :]
                for k in range(half)
            ],
            axis=0,
        )
        sides = []
        for s in range(levs):
            pieces = []
            for v in range(lanes // LANES):
                lane = slice(v * LANES, (v + 1) * LANES)
                north, south = [
                    jnp.concatenate([all_ref[s, k, span_of(part), lane] for k in order], axis=0)
                    for order in (range(half), [shards - 1 - k for k in range(half)])
                ]
                north = north.astype(F32)
                south = south.astype(F32)
                even = (weights * (north + south)).astype(BF16)
                odd = (weights * (north - south)).astype(BF16)
                pieces.append(jnp.concatenate([even, odd], axis=0).T)
            sides.append(jnp.concatenate(pieces, axis=0))
        for m in range(local_waves):
            for c in range(channels):
                low = m * both_rows + c * items
                stack = jnp.concatenate([side[low : low + items] for side in sides], axis=0)
                vals = lax.dot_general(in_modes_ref[...], stack, NN, preferred_element_type=F32)
                turned_ref[part, m, c * modes : (c + 1) * modes, :] = vals.astype(BF16)
        return carry

    def work(part, carry):
        @pl.when(part + LEAD < parts)
        def _():
            start_in(part + LEAD, 0)

        arrived(land_ref, in_send, in_recv, part).wait_recv()
        own(sent_ref, land_ref, 0, part).wait()

        @pl.when(part >= FIRST)
        def _():
            pass_far(part - FIRST)

        @pl.when(part >= SECOND)
        def _():
            pass_near(part - SECOND)

        got = land_ref[:, span_of(part), :].astype(F32).reshape(shards * chunk, -1)
        for w in range(local_waves):
            in_ref[w] = take_lanes(got, w, both_rows)
        lax.fori_loop(0, chunk // GROUP, functools.partial(several, part), 0)
        made = join_lanes([out_ref[w] for w in range(local_waves)], both_rows).astype(BF16)
        leave_ref[:, span_of(part), :] = made.reshape(shards, chunk, -1)
        for away in range(1, shards):
            remote(leave_ref, back_ref, out_send, out_recv, away, part).start()
        own(leave_ref, back_ref, 1, part).start()

        @pl.when(part >= THIRD)
        def _():
            fold(part - THIRD, 0)

        return carry

    lax.fori_loop(0, parts, work, 0)

    def give(m):
        return pltpu.make_async_remote_copy(
            src_ref=give_ref.at[m],
            dst_ref=update_ref.at[m, :, :, pl.ds(start, part_span)],
            send_sem=give_send.at[m],
            recv_sem=give_recv.at[m],
            device_id={"lev": partner},
            device_id_type=pl.DeviceIdType.MESH,
        )

    part_span = span // 2
    start = pl.multiple_of(core * part_span, part_span)
    folded = max(parts - THIRD, 0)
    early = max(parts - SECOND + 2, 0)

    def forward(m, first, last):
        seat = lax.broadcasted_iota(jnp.int32, (1, part_span), 1) + start
        polys = []
        for p in range(first, last):
            leg = jnp.concatenate(
                [
                    leg_ref[m, pl.ds(k * band + p * chunk, chunk), pl.ds(start, part_span)]
                    for k in range(half)
                ],
                axis=0,
            )
            kept = jnp.broadcast_to(seat % 2 == 0, leg.shape)
            none = jnp.zeros_like(leg)
            polys += [jnp.where(kept, leg, none), jnp.where(kept, none, leg)]
        return lax.dot_general(
            jnp.concatenate([turned_ref[p, m] for p in range(first, last)], axis=1),
            jnp.concatenate(polys, axis=0),
            NN,
            preferred_element_type=F32,
        )

    def head(m, carry):
        acc_ref[m] = forward(m, 0, early)
        return carry

    def ready(turn):
        done = jnp.minimum(folded + 2 * (turn + 1), parts - SECOND + turn)
        return jnp.clip(done, folded, parts)

    def drain(turn, carry):
        @pl.when((parts - FIRST + turn >= 0) & (turn < FIRST))
        def _():
            pass_far(parts - FIRST + turn)

        @pl.when((parts - SECOND + turn >= 0) & (turn < SECOND))
        def _():
            pass_near(parts - SECOND + turn)

        if early:

            @pl.when((turn >= 3) & (turn - 3 < local_waves))
            def _():
                head(turn - 3, 0)

        lax.fori_loop(ready(turn - 1), ready(turn), fold, 0)
        return carry

    turns_left = max(SECOND, -(-(parts - folded) // 2) - 1) + 1
    lax.fori_loop(0, turns_left, drain, 0)
    if early:
        lax.fori_loop(min(turns_left - 3, local_waves), local_waves, head, 0)
    pair_rows = jnp.concatenate(
        [
            out_modes_ref[pl.ds(pl.multiple_of(r * items, items), items), :]
            for r in (lev, partner)
        ],
        axis=0,
    )

    def one(m, carry):
        seat = lax.broadcasted_iota(jnp.int32, (1, part_span), 1) + start
        values = forward(m, early, parts)
        if early:
            values = values + acc_ref[m]
        degree = (seat + all_ids[me * local_waves + m]).astype(F32)
        live = seat < all_lengths[me * local_waves + m]
        damp = 1.0 / (1.0 + depth_ref[:, :1] * degree * (degree + 1.0) / float(NT * NT))
        damp = jnp.where(live, damp, 0.0)
        for c in range(channels):
            scaled = (values[c * modes : (c + 1) * modes] * damp).astype(BF16)
            mixed = lax.dot_general(pair_rows, scaled, NN, preferred_element_type=F32)
            mixed = mixed.astype(BF16)
            update_ref[m, c, :, pl.ds(start, part_span)] = mixed[:items]
            give_ref[m, c] = mixed[items:]
        give(m).start()
        return carry

    lax.fori_loop(0, local_waves, one, 0)

    departed(sent_ref, in_send, in_recv).wait_send()
    departed(leave_ref, out_send, out_recv).wait_send()

    def finish(part, carry):
        for away in range(1, chips):
            far(away, part).wait_send()
        for away in range(chips):
            near(away, part).wait_send()
        return carry

    lax.fori_loop(0, parts, finish, 0)

    def given(m, carry):
        give(m).wait()
        return carry

    lax.fori_loop(0, local_waves, given, 0)


def on_device(
    spectral,
    legendre,
    wave_ids,
    trunc_lengths,
    cycle_points,
    grid_coef,
    cycle_weights,
    modes_in,
    modes_out,
    depths,
):
    shards = lax.axis_size("wave")
    levs = lax.axis_size("lev")
    chips = levs // 2
    waves, channels, items, span = spectral.shape
    half_lat = legendre.shape[1]
    rows = channels * items
    band = grid_coef.shape[0]
    modes = modes_in.shape[0]
    lanes = pad_to(waves * rows, LANES)
    chunk = next(c for c in (16, 8) if band % c == 0)
    stride = next(c * chunk for c in (2, 1) if band % (c * chunk) == 0)
    parts = band // chunk
    messages = (shards, band, lanes)
    vmem = pl.BlockSpec(memory_space=pltpu.VMEM)
    smem = pl.BlockSpec(memory_space=pltpu.SMEM)
    hbm = pl.BlockSpec(memory_space=pltpu.HBM)
    dma = pltpu.SemaphoreType.DMA
    return pl.pallas_call(
        functools.partial(trip_kernel, chunk, stride),
        name="trip",
        out_shape=jax.ShapeDtypeStruct(spectral.shape, BF16),
        in_specs=[smem] * 3 + [hbm] * 3 + [vmem] * 4,
        out_specs=vmem,
        scratch_shapes=[
            pltpu.VMEM(spectral.shape, BF16),
            pltpu.VMEM(legendre.shape, BF16),
            pltpu.VMEM(grid_coef.shape, F32),
            pltpu.VMEM((waves, 2 * pad_to(rows, LANES), span), BF16),
            pltpu.VMEM(messages, BF16),
            pltpu.VMEM(messages, BF16),
            pltpu.VMEM(messages, BF16),
            pltpu.VMEM((levs, *messages), BF16),
            pltpu.VMEM((waves, shards * chunk, LANES), F32),
            pltpu.VMEM((waves, shards * chunk, LANES), F32),
            pltpu.VMEM((parts, waves, channels * modes, shards * chunk), BF16),
            pltpu.VMEM((waves, channels, items, span // 2), BF16),
            pltpu.VMEM((pad_to(half_lat, LANES), LANES), F32),
            pltpu.VMEM((modes, LANES), F32),
            pltpu.VMEM((waves, channels * modes, span // 2), F32),
            dma,
            dma((band // stride,)),
            dma,
            dma,
            dma((parts,)),
            dma,
            dma((parts,)),
            dma((max(chips - 1, 1), parts)),
            dma((max(chips - 1, 1), parts)),
            dma((chips, parts)),
            dma((chips, parts)),
            dma((2, parts)),
            dma((waves,)),
            dma((waves,)),
        ],
        compiler_params=pltpu.CompilerParams(
            vmem_limit_bytes=56 << 20, collective_id=0, has_side_effects=True
        ),
    )(
        wave_ids,
        trunc_lengths,
        cycle_points,
        spectral,
        legendre,
        grid_coef,
        jnp.pad(cycle_weights, (0, -half_lat % LANES)).reshape(-1, LANES),
        modes_in,
        modes_out,
        depths[None, :],
    )


def solution(mesh):
    placed = (
        P("wave", None, "lev", None),
        P("wave", None, None),
        P(),
        P(),
        P(),
        P("wave", None),
        P(),
        P(),
        P(),
        P(),
    )
    return jax.shard_map(
        on_device,
        mesh=mesh,
        in_specs=placed,
        out_specs=P("wave", None, "lev", None),
        check_vma=False,
    )
```
